32 devices in a mesh: section: 4 (over y, x), mp: 4 (over z), dp: 2 (over core).
Axes of the slice: x: 2, y: 2, z: 4, core: 2. Of those that a mesh axis runs over, the one named last changes fastest.
Arguments:
- stream: bfloat16 [4, 64, 4096], P('dp', None, 'mp'), may hold values from -6 to 6
- cotangent: bfloat16 [4, 64, 4096], P('dp', None, 'mp'), may hold values from -6 to 6
- token_ids: int32 [4, 64], P('dp'), may hold values from 0 to 32127, as said below
- buckets: int32 [64, 64], replicated, may hold values from 0 to 31, as said below
- bias_table: float32 [32, 32], P(None, 'mp'), may hold values from -300 to 300
- gain: float32 [4, 4096], P('section'), may hold values from 0.25 to 1.75
- w_query: bfloat16 [4, 4096, 2048], P('section', None, 'mp'), may hold values from -0.01171875 to 0.01171875
- w_key: bfloat16 [4, 4096, 2048], P('section', None, 'mp'), may hold values from -0.09375 to 0.09375
- w_value: bfloat16 [4, 4096, 2048], P('section', None, 'mp'), may hold values from -0.09375 to 0.09375
- w_out: bfloat16 [4, 2048, 4096], P('section', None, 'mp'), may hold values from -0.125 to 0.125
Outputs:
- input_grads: bfloat16 [4, 4, 64, 4096], P('section', 'dp', None, 'mp')
- gain_grad: float32 [4, 4096], P('section', 'mp')
- table_grad: float32 [32, 32], P(None, 'mp')
The draws below stay inside these ranges and needn't reach their ends.
Inputs may be any that keep to these rules, and one draw needn't show every extreme that they name: `token_ids`: in each sequence the ids are nonzero up to a length of 32 or more and zero after it. `buckets`: the bucket of a query and a key depends only on the key's position minus the query's: below 16 for keys at or before the query, 16 or more for keys after it.
All inputs are finite; a program needn't handle non-finite values.
Results may differ from the reference program's by a relative error of at most 0.035.
Values may be sent and summed in bfloat16 or wider, within the bound.
A program may use at most 64 MiB of HBM per device.

```python
import jax
import jax.numpy as jnp
from jax import lax

D = 4096
HEADS = 32
HD = 64
BUCKETS = 32
VOCAB = 32128
SEQ = 64
LAYERS = 4
BATCH = 4
INNER = 2048
N_SECTION = 4
N_MP = 4


def draw_token_ids(key, part):
    id_key = jax.random.fold_in(key, 11)
    length_key = jax.random.fold_in(key, 12)
    drawn_ids = jax.random.randint(id_key, (BATCH, SEQ), 1, VOCAB, dtype=jnp.int32)
    lengths = jax.random.randint(length_key, (BATCH, 1), SEQ // 2, SEQ + 1, dtype=jnp.int32)
    positions = jnp.arange(SEQ, dtype=jnp.int32)[None, :]
    return jnp.where(positions < lengths, drawn_ids, 0).astype(jnp.int32)


def draw_buckets(key, part):
    exact_key = jax.random.fold_in(key, 21)
    step_key = jax.random.fold_in(key, 22)
    half_count = BUCKETS // 2
    exact_count = jax.random.randint(exact_key, (), 2, 9, dtype=jnp.int32)
    widened = jax.random.randint(step_key, (half_count - 1,), 1, 3 + SEQ // 32, dtype=jnp.int32)
    levels = jnp.arange(half_count - 1, dtype=jnp.int32)
    step_sizes = jnp.where(levels < exact_count - 1, 1, widened)
    bounds = jnp.cumsum(step_sizes)
    offsets = jnp.arange(SEQ, dtype=jnp.int32)[None, :] - jnp.arange(SEQ, dtype=jnp.int32)[:, None]
    distance = jnp.abs(offsets)
    level_index = jnp.sum((distance[:, :, None] >= bounds[None, None, :]).astype(jnp.int32), axis=2)
    return jnp.where(offsets > 0, half_count + level_index, level_index).astype(jnp.int32)


def draw_bias_table(key, part):
    table_key = jax.random.fold_in(key, 31)
    return (1.5 * jax.random.truncated_normal(table_key, -4.0, 4.0, (BUCKETS, HEADS), jnp.float32)).astype(jnp.float32)


def block_scale(key, shape, cuts, smallest, top_value):
    level, own = 1.0, jax.random.fold_in(key, 6)
    for axis_at, blocks in cuts:
        heights = jnp.exp(jax.random.uniform(jax.random.fold_in(own, axis_at), (blocks,), jnp.float32, smallest / len(cuts), top_value / len(cuts)))
        level = level * jnp.repeat(heights, shape[axis_at] // blocks).reshape([-1 if axis == axis_at else 1 for axis in range(len(shape))])
    return level


def centred(own_key, shape, scale, most, pieces=(), held_as=jnp.bfloat16):
    loudness = block_scale(own_key, shape, pieces, -0.22, 0.18) if pieces else 1.0
    array = jax.random.normal(own_key, shape, jnp.float32) * scale * loudness
    return jnp.minimum(jnp.maximum(array, -most), most).astype(held_as)


def setup_inputs(seed: int = 0) -> dict:
    arg_keys = jax.random.split(jax.random.key(seed), 11)
    return {
        "stream": centred(arg_keys[0], (BATCH, SEQ, D), 1.0, 6.0, ((0, 2), (2, 4))),
        "cotangent": centred(arg_keys[1], (BATCH, SEQ, D), 1.0, 6.0, ((0, 2), (2, 4))),
        "token_ids": draw_token_ids(jax.random.fold_in(arg_keys[10], 71), 0),
        "buckets": draw_buckets(jax.random.fold_in(arg_keys[10], 71), 0),
        "bias_table": draw_bias_table(jax.random.fold_in(arg_keys[10], 71), 0),
        "gain": jnp.clip(1.0 + 0.15 * jax.random.normal(arg_keys[5], (LAYERS, D), jnp.float32), 0.25, 1.75),
        "w_query": centred(arg_keys[6], (LAYERS, D, INNER), (D * HD) ** -0.5, 0.01171875, ((0, 4), (2, 4))),
        "w_key": centred(arg_keys[7], (LAYERS, D, INNER), D ** -0.5, 0.09375, ((0, 4), (2, 4))),
        "w_value": centred(arg_keys[8], (LAYERS, D, INNER), D ** -0.5, 0.09375, ((0, 4), (2, 4))),
        "w_out": centred(arg_keys[9], (LAYERS, INNER, D), INNER ** -0.5, 0.125, ((0, 4), (2, 4))),
    }


neg_fill = -1000000000.0
epsilon = 1e-06

def round_half(values):
    return lax.optimization_barrier(values.astype(jnp.bfloat16)).astype(jnp.float32)

def attend(proj_rows, bias_heads, mask_row):
    inner_width = HEADS * HD
    proj_f32 = proj_rows.astype(jnp.float32)
    queries = proj_f32[:, :inner_width].reshape(SEQ, HEADS, HD)
    key_rows = proj_f32[:, inner_width:2 * inner_width].reshape(SEQ, HEADS, HD)
    values = proj_f32[:, 2 * inner_width:].reshape(SEQ, HEADS, HD)
    scores = jnp.einsum('qhd,khd->hqk', queries, key_rows) + bias_heads + mask_row[None, None, :]
    row_max = lax.optimization_barrier(jnp.max(scores, axis=-1, keepdims=True))
    exp_scores = jnp.exp(scores - row_max)
    prob_full = exp_scores / lax.optimization_barrier(jnp.sum(exp_scores, axis=-1, keepdims=True))
    mixed_rows = jnp.einsum('hqk,khd->qhd', round_half(prob_full), values)
    return (mixed_rows.reshape(SEQ, inner_width).astype(jnp.bfloat16), prob_full)

def forward_layer(rows, mask_row, gain_row, w_joined, w_output, bias_heads):
    rows_f32 = rows.astype(jnp.float32)
    inv_rms = lax.rsqrt(lax.optimization_barrier(jnp.sum(rows_f32 * rows_f32, axis=1, keepdims=True)) / D + epsilon)
    scaled = (rows_f32 * gain_row[None, :]).astype(jnp.bfloat16)
    raw_proj = jnp.dot(scaled, w_joined, preferred_element_type=jnp.float32)
    proj_rows = (raw_proj * inv_rms).astype(jnp.bfloat16)
    mixed_rows, prob_full = attend(proj_rows, bias_heads, mask_row)
    branch_out = jnp.dot(mixed_rows, w_output, preferred_element_type=jnp.float32)
    next_rows = (rows_f32 + branch_out).astype(jnp.bfloat16)
    return (next_rows, (inv_rms, raw_proj, proj_rows, prob_full))

def backward_layer(upstream, rows, kept, gain_row, w_joined, w_output):
    inv_rms, raw_proj, proj_rows, prob_full = kept
    inner_width = HEADS * HD
    share_width = D // N_MP
    group_width = inner_width // N_MP
    up_blocks = upstream.astype(jnp.float32).reshape(SEQ, N_MP, share_width)
    out_blocks = w_output.astype(jnp.float32).reshape(inner_width, N_MP, share_width)
    head_parts = jnp.einsum('sjc,ijc->jsi', up_blocks, out_blocks)
    mixed_grad = lax.optimization_barrier(jnp.sum(round_half(head_parts), axis=0))
    mixed_half = round_half(mixed_grad).reshape(SEQ, HEADS, HD)
    proj_f32 = proj_rows.astype(jnp.float32)
    queries = proj_f32[:, :inner_width].reshape(SEQ, HEADS, HD)
    key_rows = proj_f32[:, inner_width:2 * inner_width].reshape(SEQ, HEADS, HD)
    values = proj_f32[:, 2 * inner_width:].reshape(SEQ, HEADS, HD)
    prob_grad = jnp.einsum('qhd,khd->hqk', mixed_half, values)
    value_grad = jnp.einsum('hqk,qhd->khd', round_half(prob_full), mixed_half)
    score_grad = prob_full * (prob_grad - lax.optimization_barrier(jnp.sum(prob_grad * prob_full, axis=-1, keepdims=True)))
    score_half = round_half(score_grad)
    query_grad = jnp.einsum('hqk,khd->qhd', score_half, key_rows)
    key_grad = jnp.einsum('hqk,qhd->khd', score_half, queries)
    proj_grad = jnp.concatenate([query_grad.reshape(SEQ, inner_width), key_grad.reshape(SEQ, inner_width), value_grad.reshape(SEQ, inner_width)], axis=1)
    radial_sum = lax.optimization_barrier(jnp.sum(proj_grad * raw_proj, axis=1, keepdims=True))
    scaled_grad = round_half(proj_grad * inv_rms).reshape(SEQ, 3, N_MP, group_width)
    joined_blocks = w_joined.astype(jnp.float32).reshape(D, 3, N_MP, group_width)
    input_parts = jnp.einsum('scjx,dcjx->jsd', scaled_grad, joined_blocks)
    normed_grad = lax.optimization_barrier(jnp.sum(round_half(input_parts), axis=0))
    rows_f32 = rows.astype(jnp.float32)
    input_grad = (upstream.astype(jnp.float32) + normed_grad * gain_row[None, :] - radial_sum * inv_rms ** 3 / D * rows_f32).astype(jnp.bfloat16)
    gain_part = lax.optimization_barrier(jnp.sum(normed_grad * rows_f32, axis=0))
    return (input_grad, gain_part, score_grad)

def reference(stream, cotangent, token_ids, buckets, bias_table, gain, w_query, w_key, w_value, w_out):
    bias_heads = jnp.transpose(bias_table[buckets], (2, 0, 1))
    key_masks = jnp.where(token_ids == 0, neg_fill, 0.0).astype(jnp.float32)
    layer_inputs = []
    layer_kept = []
    rows = stream
    for layer_index in range(N_SECTION):
        w_joined = jnp.concatenate([w_query[layer_index], w_key[layer_index], w_value[layer_index]], axis=1)

        def forward_one(pair, layer_index=layer_index, w_joined=w_joined):
            return forward_layer(pair[0], pair[1], gain[layer_index], w_joined, w_out[layer_index], bias_heads)
        next_rows, kept = lax.map(forward_one, (rows, key_masks))
        layer_inputs.append(rows)
        layer_kept.append(kept)
        rows = next_rows
    upstream = cotangent
    grads_list = [None] * N_SECTION
    gain_list = [None] * N_SECTION
    score_total = jnp.zeros((HEADS, SEQ, SEQ), jnp.float32)
    for layer_index in reversed(range(N_SECTION)):
        w_joined = jnp.concatenate([w_query[layer_index], w_key[layer_index], w_value[layer_index]], axis=1)

        def backward_one(packed, layer_index=layer_index, w_joined=w_joined):
            return backward_layer(packed[0], packed[1], packed[2], gain[layer_index], w_joined, w_out[layer_index])
        input_grad, gain_parts, score_grads = lax.map(backward_one, (upstream, layer_inputs[layer_index], layer_kept[layer_index]))
        grads_list[layer_index] = input_grad
        gain_list[layer_index] = lax.optimization_barrier(jnp.sum(gain_parts, axis=0))
        score_total = score_total + lax.optimization_barrier(jnp.sum(score_grads, axis=0))
        upstream = input_grad
    onehot = (buckets[:, :, None] == jnp.arange(BUCKETS, dtype=jnp.int32)[None, None, :]).astype(jnp.float32)
    table_grad = jnp.einsum('qkb,hqk->bh', onehot, score_total, precision=lax.Precision.HIGHEST)
    return (jnp.stack(grads_list), jnp.stack(gain_list), table_grad)
```

```python
import functools

import jax
import jax.numpy as jnp
from jax import lax
from jax.experimental import pallas as pl
from jax.experimental.pallas import tpu as pltpu
from jax.sharding import PartitionSpec as P

neg_fill = -1000000000.0
epsilon = 1e-06
MESH = pl.DeviceIdType.MESH
DELAY = 8000
DELAYED = 1
f32 = jnp.float32
bf16 = jnp.bfloat16


def dot_nn(a, b):
    return lax.dot_general(a, b, (((1,), (0,)), ((), ())), preferred_element_type=f32)


def dot_nt(a, b):
    return lax.dot_general(a, b, (((1,), (1,)), ((), ())), preferred_element_type=f32)


def dot_tn(a, b):
    return lax.dot_general(a, b, (((0,), (0,)), ((), ())), preferred_element_type=f32)


def relay_kernel(
    sections, n, dps, head_dim,
    stream, cotangent, tokens, buckets, table, gain, wq_hbm, wk_hbm, wv_hbm, wo_hbm,
    grads_out, gain_out, table_out,
    wq, wk, wv, wo, bias, xin, mixg, hp, ip, rad, gin, hs, ins, rads, share, grad,
    raw, proj, probs, inv_kept, acc, mg_ref, sgr, sq, diag, tab, gains, ex_h, ex_i,
    w_sem, l_sem, x_s, y_s, x_r, m_s, m_r, h_s, h_r, i_s, i_r, r_s, r_r, g_s, g_r, t_s, t_r, d_s, d_r, fx_s, fm_s, eh_r, ei_r,
):
    micro, seq, width = stream.shape
    heads = bias.shape[0]
    inner = heads * head_dim
    per = 128 // head_dim
    groups = heads // per
    model_width = n * width
    sec = lax.axis_index("section")
    me = lax.axis_index("mp")
    dp = lax.axis_index("dp")
    everyone = sections * dps
    mine = sec * dps + dp
    turn = 1 - 2 * (me // ((n + 1) // 2))

    def peer(i):
        return (me + i * turn + n) % n

    relayed = n == 4
    inner_chip = (me % (n - 1)) != 0 if relayed else True

    def visit(at):
        return jnp.where(at == 1, 2, jnp.where(at == 2, 1, at)) if relayed else at

    def unless_far(i, act):
        if relayed:
            pl.when((i < n - 1) | inner_chip)(act)
        else:
            act()

    def remote(src, dst, ssem, rsem, to_sec, to_mp):
        return pltpu.make_async_remote_copy(
            src_ref=src, dst_ref=dst, send_sem=ssem, recv_sem=rsem,
            device_id={"section": to_sec, "mp": to_mp}, device_id_type=MESH,
        )

    loads = [
        pltpu.make_async_copy(src, dst, w_sem.at[at])
        for at, (src, dst) in enumerate(
            ((wq_hbm.at[0], wq), (wk_hbm.at[0], wk), (wv_hbm.at[0], wv), (wo_hbm.at[0], wo))
        )
    ]
    for load in loads:
        load.start()

    barrier = pltpu.get_barrier_semaphore()
    is_first = sec == 0
    is_last = sec == sections - 1
    for i in range(1, n):
        pl.semaphore_signal(
            barrier, inc=1, device_id={"section": sec, "mp": peer(i)}, device_id_type=MESH
        )

    @pl.when(sec > 0)
    def _():
        for j in range(n):
            pl.semaphore_signal(
                barrier, inc=1, device_id={"section": sec - 1, "mp": j}, device_id_type=MESH
            )

    @pl.when(sec < sections - 1)
    def _():
        for j in range(n):
            pl.semaphore_signal(
                barrier, inc=1, device_id={"section": sec + 1, "mp": j}, device_id_type=MESH
            )

    def member(i):
        return (mine + i) % everyone

    for i in range(1, everyone):
        other = member(i)
        pl.semaphore_signal(
            barrier, inc=1, device_id={"section": other // dps, "dp": other % dps},
            device_id_type=MESH,
        )

    greeters = n - 1 + everyone - 1 + n * jnp.minimum(sec, 1) + n * jnp.minimum(sections - 1 - sec, 1)
    pl.semaphore_wait(barrier, greeters)

    def x_copy(m, j):
        return remote(stream.at[m], xin.at[m, me], x_s.at[m, j], x_r.at[m, me], sec, j)

    def y_copy(m, j):
        return remote(share.at[m], xin.at[m, me], y_s.at[m, j], x_r.at[m, me], sec + 1, j)

    def send_x(m):
        pltpu.make_async_copy(stream.at[m], xin.at[m, me], l_sem.at[m]).start()
        for i in range(n - 1, 0, -1):
            unless_far(i, lambda i=i: x_copy(m, peer(i)).start())

    @pl.when(is_first)
    def _():
        @pl.when(dp % 2 == DELAYED)
        def _():
            pl.delay(DELAY)

        send_x(0)

    def head_bias(h, carry):
        value = jnp.zeros((seq, seq), f32)
        held = buckets[...]
        for c in range(table.shape[1]):
            value = jnp.where(held == c, table[h, c], value)
        bias[h] = value
        return carry

    lax.fori_loop(0, heads, head_bias, 0)
    tab[mine] = jnp.zeros(tab.shape[1:], f32)
    diag[...] = jnp.zeros(diag.shape, f32)
    gains[dp] = jnp.zeros(gains.shape[1:], f32)
    for load in loads:
        load.wait()

    def h_copy(m, j):
        return remote(hs.at[m, j], hp.at[m, me], h_s.at[m, j], h_r.at[m, me], sec, j)

    def emit(at):
        return jnp.where(at == 0, 3, jnp.where(at == 3, 2, 2 - at)) if relayed else n - 1 - at

    def pass_on(m, i, part, own, extra, own_sem, extra_sem, copy):
        j = peer(i)
        own[m, j] = part.astype(bf16)
        if not relayed:
            pl.when(i > 0)(lambda: copy(m, j).start())
            return

        def hand_over():
            return remote(own.at[m, j], extra.at[m], own_sem.at[m, j], extra_sem.at[m], sec, peer(1))

        @pl.when((i == n - 2) & inner_chip)
        def _():
            hand_over().wait_recv()
            own[m, j] = (part + extra[m].astype(f32)).astype(bf16)

        @pl.when((i > 0) & ((i < n - 1) | inner_chip))
        def _():
            copy(m, j).start()

        @pl.when((i == n - 1) & ((me % (n - 1)) == 0))
        def _():
            hand_over().start()

    def head_parts(m, upstream):
        def one(step, carry):
            i = emit(step)
            j = peer(i)
            rows = wo[pl.ds(pl.multiple_of(j * inner, inner), inner), :]
            pass_on(m, i, dot_nt(upstream[m], rows), hs, ex_h, h_s, eh_r, h_copy)

            return carry

        lax.fori_loop(0, n, one, 0)

    @pl.when(is_last)
    def _():
        def one(m, carry):
            head_parts(m, cotangent)
            return carry

        lax.fori_loop(0, micro, one, 0)

    lane = lax.broadcasted_iota(jnp.int32, (1, 128), 1)
    picks = [
        jnp.where((lane // head_dim) == e, 1.0, 0.0).astype(f32) for e in range(per)
    ]
    picks_half = [pick.astype(bf16) for pick in picks]

    def spread(block):
        return jnp.concatenate([block * pick for pick in picks_half], axis=0)

    def fold(block):
        total = block[:seq] * picks[0]
        for e in range(1, per):
            total = total + block[e * seq : (e + 1) * seq] * picks[e]
        return total

    def mix_copy(m, j):
        return remote(mixg.at[m, me], mixg.at[m, me], m_s.at[m, j], m_r.at[m, me], sec, j)

    def on_x(m, j):
        return remote(xin.at[m, j], xin.at[m, j], fx_s.at[m], x_r.at[m, j], sec, peer(n - 1))

    def on_mix(m, j):
        return remote(mixg.at[m, j], mixg.at[m, j], fm_s.at[m], m_r.at[m, j], sec, peer(n - 1))

    def forward(m):
        @pl.when(is_first)
        def _():
            pltpu.make_async_copy(stream.at[m], xin.at[m, me], l_sem.at[m]).wait()

        raw[m] = jnp.zeros(raw.shape[1:], f32)
        sq[...] = jnp.zeros(sq.shape, f32)

        def gathered(at, inside):
            i = visit(at)
            j = peer(i)

            @pl.when((sec > 0) | (i > 0))
            def _():
                remote(
                    share.at[m], xin.at[m, j], x_s.at[m, j], x_r.at[m, j], sec, j
                ).wait_recv()

            if relayed:

                @pl.when((i == n - 2) & inner_chip)
                def _():
                    on_x(m, j).start()

            piece = xin[m, j].astype(f32)
            sq[...] += jnp.sum(piece * piece, axis=1, keepdims=True)
            cols = pl.ds(pl.multiple_of(j * width, width), width)
            scaled = (piece * gain[:, cols]).astype(bf16)
            rows = pl.ds(pl.multiple_of(j * width, width), width)
            for at, w in enumerate((wq, wk, wv)):
                raw[m, :, at * inner : (at + 1) * inner] += dot_nn(scaled, w[rows, :])
            return inside

        lax.fori_loop(0, n, gathered, 0)
        inv = lax.rsqrt(sq[:, :1] / model_width + epsilon)
        inv_kept[m] = jnp.broadcast_to(inv, (seq, 128))
        proj[m] = (raw[m] * inv).astype(bf16)
        mask_row = jnp.where(tokens[pl.ds(m, 1), :] == 0, neg_fill, 0.0)
        for p in range(groups):
            cols = slice(p * 128, (p + 1) * 128)
            q = proj[m, :, p * 128 : (p + 1) * 128]
            k = proj[m, :, inner + p * 128 : inner + (p + 1) * 128]
            v = proj[m, :, 2 * inner + p * 128 : 2 * inner + (p + 1) * 128]
            scores = dot_nt(spread(q), k)
            scores = scores + bias[p * per : (p + 1) * per].reshape(per * seq, seq) + mask_row
            top = jnp.max(scores, axis=-1, keepdims=True)
            grown = jnp.exp(scores - top)
            prob = grown / jnp.sum(grown, axis=-1, keepdims=True)
            probs[m, p] = prob
            mixg[m, me, :, cols] = fold(dot_nn(prob.astype(bf16), v)).astype(bf16)

        @pl.when(sec < sections - 1)
        def _():
            for i in range(n - 1, 0, -1):
                unless_far(i, lambda i=i: mix_copy(m, peer(i)).start())

        @pl.when(is_first & (m + 1 < micro))
        def _():
            send_x(m + 1)

    def project(m):
        @pl.when(sec < sections - 1)
        def _():
            acc[...] = xin[m, me].astype(f32)

            def mixed(at, inside):
                i = visit(at)
                j = peer(i)

                @pl.when(i > 0)
                def _():
                    remote(
                        mixg.at[m, j], mixg.at[m, j], m_s.at[m, j], m_r.at[m, j], sec, j
                    ).wait_recv()

                if relayed:

                    @pl.when((i == n - 2) & inner_chip)
                    def _():
                        on_mix(m, j).start()

                rows = pl.ds(pl.multiple_of(j * inner, inner), inner)
                acc[...] += dot_nn(mixg[m, j], wo[rows, :])
                return inside

            lax.fori_loop(0, n, mixed, 0)
            share[m] = acc[...].astype(bf16)
            for i in range(n - 1, -1, -1):
                unless_far(i, lambda i=i: y_copy(m, peer(i)).start())

    def i_copy(m, j):
        return remote(ins.at[m, j], ip.at[m, me], i_s.at[m, j], i_r.at[m, me], sec, j)

    def r_copy(m, j):
        return remote(rads.at[m], rad.at[m, me], r_s.at[m, j], r_r.at[m, me], sec, j)

    def g_copy(m, to_sec):
        return remote(grad.at[m], gin.at[m], g_s.at[m], g_r.at[m], to_sec, me)

    def t_copy(i):
        other = member(i)
        return pltpu.make_async_remote_copy(
            src_ref=tab.at[mine], dst_ref=tab.at[mine],
            send_sem=t_s.at[other], recv_sem=t_r.at[mine],
            device_id={"section": other // dps, "dp": other % dps}, device_id_type=MESH,
        )

    def d_copy(i):
        other = (dp + i) % dps
        return pltpu.make_async_remote_copy(
            src_ref=gains.at[dp], dst_ref=gains.at[dp],
            send_sem=d_s.at[other], recv_sem=d_r.at[dp],
            device_id={"dp": other}, device_id_type=MESH,
        )

    def receive(m):
        g_copy(m, sec + 1).wait_recv()
        head_parts(m, gin)

    def backward(m):
        @pl.when(is_last)
        def _():
            gin[m] = cotangent[m]

        mg_ref[...] = hs[m, me].astype(f32)

        def arrived(i, inside):
            j = peer(i)

            def add():
                remote(hs.at[m, j], hp.at[m, j], h_s.at[m, j], h_r.at[m, j], sec, j).wait_recv()
                mg_ref[...] += hp[m, j].astype(f32)

            unless_far(i, add)
            return inside

        lax.fori_loop(1, n, arrived, 0)
        inv = inv_kept[m][:, :1]
        radial = jnp.zeros((seq, 128), f32)
        for p in range(groups):
            q_cols = slice(p * 128, (p + 1) * 128)
            k_cols = slice(inner + p * 128, inner + (p + 1) * 128)
            v_cols = slice(2 * inner + p * 128, 2 * inner + (p + 1) * 128)
            q2 = spread(proj[m, :, q_cols])
            k = proj[m, :, k_cols]
            v = proj[m, :, v_cols]
            mg2 = spread(mg_ref[:, q_cols].astype(bf16))
            prob = probs[m, p]
            prob_grad = dot_nt(mg2, v)
            value_grad = dot_tn(prob.astype(bf16), mg2)
            score_grad = prob * (prob_grad - jnp.sum(prob_grad * prob, axis=-1, keepdims=True))
            wide = jnp.concatenate([score_grad, jnp.zeros_like(score_grad)], axis=1)
            for e in range(per):
                part = wide[e * seq : e * seq + 8]
                for a in range(8, seq, 8):
                    part = part + pltpu.roll(
                        wide[e * seq + a : e * seq + a + 8], (2 * seq - a) % (2 * seq), 1
                    )
                diag[p * per + e] += part
            half = score_grad.astype(bf16)
            query_grad = fold(dot_nn(half, k))
            key_grad = dot_tn(half, q2)
            for cols, part in ((q_cols, query_grad), (k_cols, key_grad), (v_cols, value_grad)):
                radial = radial + part * raw[m, :, cols]
                sgr[:, cols] = (part * inv).astype(bf16)
        rads[m] = jnp.broadcast_to(jnp.sum(radial, axis=1, keepdims=True), (seq, 128)).T[:8]
        for i in range(n - 1, 0, -1):
            r_copy(m, peer(i)).start()

        def input_part(step, inside):
            i = emit(step)
            j = peer(i)
            rows = pl.ds(pl.multiple_of(j * width, width), width)
            part = dot_nt(sgr[:, :inner], wq[rows, :])
            part += dot_nt(sgr[:, inner : 2 * inner], wk[rows, :])
            part += dot_nt(sgr[:, 2 * inner :], wv[rows, :])
            pass_on(m, i, part, ins, ex_i, i_s, ei_r, i_copy)
            return inside

        lax.fori_loop(0, n, input_part, 0)

        @pl.when(m == micro - 1)
        def _():
            sub = lax.broadcasted_iota(jnp.int32, (8, 2 * seq), 0)
            for h in range(heads):
                part = diag[h]
                for bit in (1, 2, 4):
                    moved = pltpu.roll(part, 2 * seq - bit, 1)
                    part = jnp.where((sub // bit) % 2 == 1, moved, part)
                tab[mine, h : h + 1] = jnp.sum(part, axis=0, keepdims=True)
            for i in range(1, everyone):
                t_copy(i).start()

    def settle(m):
        inv = inv_kept[m][:, :1]
        acc[...] = ins[m, me].astype(f32)
        sq[:8, :seq] = rads[m]

        def arrived_input(i, inside):
            j = peer(i)
            remote(rads.at[m], rad.at[m, j], r_s.at[m, j], r_r.at[m, j], sec, j).wait_recv()
            sq[:8, :seq] += rad[m, j]

            def add():
                remote(ins.at[m, j], ip.at[m, j], i_s.at[m, j], i_r.at[m, j], sec, j).wait_recv()
                acc[...] += ip[m, j].astype(f32)

            unless_far(i, add)
            return inside

        lax.fori_loop(1, n, arrived_input, 0)
        radial_sum = jnp.broadcast_to(sq[:1, :seq], (128, seq)).T[:, :1]
        rows_f32 = xin[m, me].astype(f32)
        normed = acc[...]
        gain_own = gain[:, pl.ds(pl.multiple_of(me * width, width), width)]
        weight = radial_sum * inv * inv * inv / model_width
        result = (gin[m].astype(f32) + normed * gain_own - weight * rows_f32).astype(bf16)
        grad[m] = result
        grads_out[0, m] = result

        @pl.when(sec > 0)
        def _():
            g_copy(m, sec - 1).start()

        gains[dp] += jnp.sum(normed * rows_f32, axis=0, keepdims=True)

    def step(t, carry):
        u = t - 2 * micro
        kind = jnp.where(u < 0, t % 2, u % 3 + 2)
        m = jnp.where(u < 0, t // 2, u // 3)
        of_last = t % 3
        kind = jnp.where(is_last, jnp.where(of_last == 0, 0, of_last + 2), kind)
        m = jnp.where(is_last, t // 3, m)
        busy = ~is_last | (t < 3 * micro)

        for at, act in enumerate((forward, project, receive, backward, settle)):
            pl.when((kind == at) & busy)(lambda act=act: act(m))

        return carry

    lax.fori_loop(0, 5 * micro, step, 0)
    for i in range(1, dps):
        d_copy(i).start()

    def finish(m, carry):
        def one(i, inside):
            j = peer(i)
            h_copy(m, j).wait_send()
            i_copy(m, j).wait_send()
            r_copy(m, j).wait_send()

            @pl.when(is_first)
            def _():
                unless_far(i, lambda: x_copy(m, j).wait_send())

            @pl.when(sec < sections - 1)
            def _():
                unless_far(i, lambda: mix_copy(m, j).wait_send())

            return inside

        lax.fori_loop(1, n, one, 0)
        if relayed:

            @pl.when(inner_chip)
            def _():
                on_x(m, peer(n - 2)).wait_send()

            @pl.when(inner_chip & (sec < sections - 1))
            def _():
                on_mix(m, peer(n - 2)).wait_send()

        @pl.when(sec > 0)
        def _():
            g_copy(m, sec - 1).wait_send()

        return carry

    lax.fori_loop(0, micro, finish, 0)

    @pl.when(sec < sections - 1)
    def _():
        def one(m, carry):
            for i in range(n):
                unless_far(i, lambda i=i: y_copy(m, peer(i)).wait_send())
            return carry

        lax.fori_loop(0, micro, one, 0)

    def table_wait(i, carry):
        other = member(i)
        pltpu.make_async_remote_copy(
            src_ref=tab.at[mine], dst_ref=tab.at[other],
            send_sem=t_s.at[other], recv_sem=t_r.at[other],
            device_id={"section": other // dps, "dp": other % dps}, device_id_type=MESH,
        ).wait()
        return carry

    lax.fori_loop(1, everyone, table_wait, 0)
    total = tab[0]
    for at in range(1, everyone):
        total = total + tab[at]
    last = buckets[seq - 1 : seq, :]
    place = jnp.concatenate([buckets[0:1, :], last[:, seq - 1 :], last[:, : seq - 1]], axis=1)
    summed = jnp.zeros(total.shape, f32)
    for c in range(table.shape[1]):
        part = jnp.sum(jnp.where(place == c, total, 0.0), axis=1, keepdims=True)
        summed = jnp.where(lane == c, part, summed)
    table_out[...] = summed[:heads, : table_out.shape[1]]
    for i in range(1, dps):
        other = (dp + i) % dps
        pltpu.make_async_remote_copy(
            src_ref=gains.at[dp], dst_ref=gains.at[other],
            send_sem=d_s.at[other], recv_sem=d_r.at[other],
            device_id={"dp": other}, device_id_type=MESH,
        ).wait()
    total = gains[0]
    for at in range(1, dps):
        total = total + gains[at]
    gain_out[...] = total


def per_device(
    stream, cotangent, token_ids, buckets, bias_table, gain, w_query, w_key, w_value, w_out
):
    sections = lax.axis_size("section")
    n = lax.axis_size("mp")
    dps = lax.axis_size("dp")
    micro, seq, width = stream.shape
    heads = bias_table.shape[1]
    inner = w_query.shape[2]
    head_dim = inner // heads
    groups = heads * head_dim // 128
    per = 128 // head_dim
    vmem = pl.BlockSpec(memory_space=pltpu.VMEM)
    hbm = pl.BlockSpec(memory_space=pl.ANY)
    dma = pltpu.SemaphoreType.DMA
    grads, gains, table_grad = pl.pallas_call(
        functools.partial(relay_kernel, sections, n, dps, head_dim),
        out_shape=(
            jax.ShapeDtypeStruct((1, micro, seq, width), bf16),
            jax.ShapeDtypeStruct((1, width), f32),
            jax.ShapeDtypeStruct(bias_table.shape[::-1], f32),
        ),
        in_specs=[vmem, vmem, vmem, vmem, pl.BlockSpec(memory_space=pltpu.SMEM), vmem]
        + [hbm] * 4,
        out_specs=(vmem, vmem, vmem),
        scratch_shapes=[
            pltpu.VMEM(w_query.shape[1:], bf16),
            pltpu.VMEM(w_key.shape[1:], bf16),
            pltpu.VMEM(w_value.shape[1:], bf16),
            pltpu.VMEM(w_out.shape[1:], bf16),
            pltpu.VMEM((heads, seq, seq), f32),
            pltpu.VMEM((micro, n, seq, width), bf16),
            pltpu.VMEM((micro, n, seq, inner), bf16),
            pltpu.VMEM((micro, n, seq, inner), bf16),
            pltpu.VMEM((micro, n, seq, width), bf16),
            pltpu.VMEM((micro, n, 8, seq), f32),
            pltpu.VMEM((micro, seq, width), bf16),
            pltpu.VMEM((micro, n, seq, inner), bf16),
            pltpu.VMEM((micro, n, seq, width), bf16),
            pltpu.VMEM((micro, 8, seq), f32),
            pltpu.VMEM((micro, seq, width), bf16),
            pltpu.VMEM((micro, seq, width), bf16),
            pltpu.VMEM((micro, seq, 3 * inner), f32),
            pltpu.VMEM((micro, seq, 3 * inner), bf16),
            pltpu.VMEM((micro, groups, per * seq, seq), f32),
            pltpu.VMEM((micro, seq, 128), f32),
            pltpu.VMEM((seq, width), f32),
            pltpu.VMEM((seq, inner), f32),
            pltpu.VMEM((seq, 3 * inner), bf16),
            pltpu.VMEM((seq, 128), f32),
            pltpu.VMEM((heads, 8, 2 * seq), f32),
            pltpu.VMEM((sections * dps, max(heads, 8), 2 * seq), f32),
            pltpu.VMEM((dps, 1, width), f32),
            pltpu.VMEM((micro, seq, inner), bf16),
            pltpu.VMEM((micro, seq, width), bf16),
            dma((4,)),
            dma((micro,)),
        ]
        + [dma((micro, n))] * 11
        + [dma((micro,))] * 2
        + [dma((sections * dps,))] * 2
        + [dma((dps,))] * 2
        + [dma((micro,))] * 4,
        compiler_params=pltpu.CompilerParams(
            collective_id=0, has_side_effects=True, vmem_limit_bytes=60 * 1024 * 1024
        ),
    )(
        stream, cotangent, token_ids, buckets, bias_table.T, gain, w_query, w_key, w_value, w_out,
    )
    return grads, gains, table_grad.T


def solution(mesh):
    in_specs = (
        P("dp", None, "mp"),
        P("dp", None, "mp"),
        P("dp", None),
        P(),
        P(None, "mp"),
        P("section", None),
        P("section", None, "mp"),
        P("section", None, "mp"),
        P("section", None, "mp"),
        P("section", None, "mp"),
    )
    out_specs = (P("section", "dp", None, "mp"), P("section", "mp"), P(None, "mp"))
    return jax.shard_map(
        per_device, mesh=mesh, in_specs=in_specs, out_specs=out_specs, check_vma=False
    )
```

```python
import functools

import jax
import jax.numpy as jnp
from jax import lax
from jax.experimental import pallas as pl
from jax.experimental.pallas import tpu as pltpu
from jax.sharding import PartitionSpec as P

neg_fill = -1000000000.0
epsilon = 1e-06
MESH = pl.DeviceIdType.MESH
DELAY = 8000
DELAYED = 1
f32 = jnp.float32
bf16 = jnp.bfloat16


def dot_nn(a, b):
    return lax.dot_general(a, b, (((1,), (0,)), ((), ())), preferred_element_type=f32)


def dot_nt(a, b):
    return lax.dot_general(a, b, (((1,), (1,)), ((), ())), preferred_element_type=f32)


def dot_tn(a, b):
    return lax.dot_general(a, b, (((0,), (0,)), ((), ())), preferred_element_type=f32)


def relay_kernel(
    sections, n, dps, head_dim,
    stream, cotangent, tokens, buckets, table, gain, wq_hbm, wk_hbm, wv_hbm, wo_hbm,
    grads_out, gain_out, table_out,
    wq, wk, wv, wo, wq_t, wk_t, wv_t, wo_t, bias, xin, mixg, hp, ip, rad, gin, hs, ins, rads, share, grad,
    raw, proj, probs, inv_kept, acc, mg_ref, sgr, sq, diag, tab, gains, ex_h, ex_i,
    w_sem, l_sem, x_s, y_s, x_r, m_s, m_r, h_s, h_r, i_s, i_r, r_s, r_r, g_s, g_r, t_s, t_r, d_s, d_r, fx_s, fm_s, eh_r, ei_r,
):
    micro, seq, width = stream.shape
    heads = bias.shape[0]
    inner = heads * head_dim
    per = 128 // head_dim
    groups = heads // per
    model_width = n * width
    sec = lax.axis_index("section")
    me = lax.axis_index("mp")
    dp = lax.axis_index("dp")
    everyone = sections * dps
    mine = sec * dps + dp
    turn = 1 - 2 * (me // ((n + 1) // 2))

    def peer(i):
        return (me + i * turn + n) % n

    relayed = n == 4
    chunks = 2 if relayed and inner % 256 == 0 and width % 256 == 0 else 1
    in_half, mix_half = width // chunks, inner // chunks

    def in_cols(c):
        return pl.ds(pl.multiple_of(c * in_half, in_half), in_half)

    def mix_cols(c):
        return pl.ds(pl.multiple_of(c * mix_half, mix_half), mix_half)

    def flip(src, dst):
        rows = min(256, src.shape[0])

        def one(r, carry):
            at = pl.ds(pl.multiple_of(r * rows, rows), rows)
            dst[:, at] = src[at, :].T
            return carry

        lax.fori_loop(0, src.shape[0] // rows, one, 0)

    def flip_all():
        for src, dst in ((wo, wo_t), (wq, wq_t), (wk, wk_t), (wv, wv_t)):
            flip(src, dst)

    flips_first = sec * 2 >= sections
    inner_chip = (me % (n - 1)) != 0 if relayed else True

    def visit(at):
        return jnp.where(at == 1, 2, jnp.where(at == 2, 1, at)) if relayed else at

    def unless_far(i, act):
        if relayed:
            pl.when((i < n - 1) | inner_chip)(act)
        else:
            act()

    def remote(src, dst, ssem, rsem, to_sec, to_mp):
        return pltpu.make_async_remote_copy(
            src_ref=src, dst_ref=dst, send_sem=ssem, recv_sem=rsem,
            device_id={"section": to_sec, "mp": to_mp}, device_id_type=MESH,
        )

    loads = [
        pltpu.make_async_copy(src, dst, w_sem.at[at])
        for at, (src, dst) in enumerate(
            ((wq_hbm.at[0], wq), (wk_hbm.at[0], wk), (wv_hbm.at[0], wv), (wo_hbm.at[0], wo))
        )
    ]
    for load in loads:
        load.start()

    barrier = pltpu.get_barrier_semaphore()
    is_first = sec == 0
    is_last = sec == sections - 1
    for i in range(1, n):
        pl.semaphore_signal(
            barrier, inc=1, device_id={"section": sec, "mp": peer(i)}, device_id_type=MESH
        )

    @pl.when(sec > 0)
    def _():
        for j in range(n):
            pl.semaphore_signal(
                barrier, inc=1, device_id={"section": sec - 1, "mp": j}, device_id_type=MESH
            )

    @pl.when(sec < sections - 1)
    def _():
        for j in range(n):
            pl.semaphore_signal(
                barrier, inc=1, device_id={"section": sec + 1, "mp": j}, device_id_type=MESH
            )

    def member(i):
        return (mine + i) % everyone

    for i in range(1, everyone):
        other = member(i)
        pl.semaphore_signal(
            barrier, inc=1, device_id={"section": other // dps, "dp": other % dps},
            device_id_type=MESH,
        )

    greeters = n - 1 + everyone - 1 + n * jnp.minimum(sec, 1) + n * jnp.minimum(sections - 1 - sec, 1)
    pl.semaphore_wait(barrier, greeters)

    def x_copy(m, j, c):
        return remote(
            stream.at[m, :, in_cols(c)], xin.at[m, me, :, in_cols(c)],
            x_s.at[m, j, c], x_r.at[m, me, c], sec, j,
        )

    def y_copy(m, j, c):
        return remote(
            share.at[m, :, in_cols(c)], xin.at[m, me, :, in_cols(c)],
            y_s.at[m, j, c], x_r.at[m, me, c], sec + 1, j,
        )

    def send_x(m):
        pltpu.make_async_copy(stream.at[m], xin.at[m, me], l_sem.at[m]).start()
        for c in range(chunks):
            for i in range(n - 1, 0, -1):
                unless_far(i, lambda i=i, c=c: x_copy(m, peer(i), c).start())

    @pl.when(is_first)
    def _():
        @pl.when(dp % 2 == DELAYED)
        def _():
            pl.delay(DELAY)

        send_x(0)

    def head_bias(h, carry):
        value = jnp.zeros((seq, seq), f32)
        held = buckets[...]
        for c in range(table.shape[1]):
            value = jnp.where(held == c, table[h, c], value)
        bias[h] = value
        return carry

    lax.fori_loop(0, heads, head_bias, 0)
    tab[mine] = jnp.zeros(tab.shape[1:], f32)
    diag[...] = jnp.zeros(diag.shape, f32)
    gains[dp] = jnp.zeros(gains.shape[1:], f32)
    for load in loads:
        load.wait()
    pl.when(flips_first)(flip_all)

    def h_copy(m, j, c):
        return remote(
            hs.at[m, j, :, mix_cols(c)], hp.at[m, me, :, mix_cols(c)],
            h_s.at[m, j, c], h_r.at[m, me, c], sec, j,
        )

    def emit(at):
        return jnp.where(at == 0, 3, jnp.where(at == 3, 2, 2 - at)) if relayed else n - 1 - at

    def pass_on(m, i, c, cols, part, own, extra, own_sem, extra_sem, copy):
        j = peer(i)
        own[m, j, :, cols] = part.astype(bf16)
        if not relayed:
            pl.when(i > 0)(lambda: copy(m, j, c).start())
            return

        def hand_over():
            return remote(
                own.at[m, j, :, cols], extra.at[m, :, cols],
                own_sem.at[m, j, c], extra_sem.at[m, c], sec, peer(1),
            )

        @pl.when((i == n - 2) & inner_chip)
        def _():
            hand_over().wait_recv()
            own[m, j, :, cols] = (part + extra[m, :, cols].astype(f32)).astype(bf16)

        @pl.when((i > 0) & ((i < n - 1) | inner_chip))
        def _():
            copy(m, j, c).start()

        @pl.when((i == n - 1) & ((me % (n - 1)) == 0))
        def _():
            hand_over().start()

    def head_parts(m, upstream):
        def one(step, carry):
            i = emit(step)
            j = peer(i)
            cols = pl.ds(pl.multiple_of(j * inner, inner), inner)
            part = dot_nn(upstream[m], wo_t[:, cols])
            for c in range(chunks):
                at = slice(c * mix_half, (c + 1) * mix_half)
                pass_on(m, i, c, at, part[:, at], hs, ex_h, h_s, eh_r, h_copy)
            return carry

        lax.fori_loop(0, n, one, 0)

    @pl.when(is_last)
    def _():
        def one(m, carry):
            head_parts(m, cotangent)
            return carry

        lax.fori_loop(0, micro, one, 0)

    lane = lax.broadcasted_iota(jnp.int32, (1, 128), 1)
    picks = [
        jnp.where((lane // head_dim) == e, 1.0, 0.0).astype(f32) for e in range(per)
    ]
    picks_half = [pick.astype(bf16) for pick in picks]

    def spread(block):
        return jnp.concatenate([block * pick for pick in picks_half], axis=0)

    def fold(block):
        total = block[:seq] * picks[0]
        for e in range(1, per):
            total = total + block[e * seq : (e + 1) * seq] * picks[e]
        return total

    def mix_copy(m, j, c):
        part = mixg.at[m, me, :, mix_cols(c)]
        return remote(part, part, m_s.at[m, j, c], m_r.at[m, me, c], sec, j)

    def on_x(m, j, c):
        part = xin.at[m, j, :, in_cols(c)]
        return remote(part, part, fx_s.at[m, c], x_r.at[m, j, c], sec, peer(n - 1))

    def on_mix(m, j, c):
        part = mixg.at[m, j, :, mix_cols(c)]
        return remote(part, part, fm_s.at[m, c], m_r.at[m, j, c], sec, peer(n - 1))

    def forward(m):
        @pl.when(is_first)
        def _():
            pltpu.make_async_copy(stream.at[m], xin.at[m, me], l_sem.at[m]).wait()

        raw[m] = jnp.zeros(raw.shape[1:], f32)
        sq[...] = jnp.zeros(sq.shape, f32)

        def gathered(step, inside):
            i = visit(step // chunks)
            j = peer(i)
            c = step % chunks

            @pl.when((sec > 0) | (i > 0))
            def _():
                remote(
                    share.at[m, :, in_cols(c)], xin.at[m, j, :, in_cols(c)],
                    x_s.at[m, j, c], x_r.at[m, j, c], sec, j,
                ).wait_recv()

            if relayed:

                @pl.when((i == n - 2) & inner_chip)
                def _():
                    on_x(m, j, c).start()

            piece = xin[m, j, :, in_cols(c)].astype(f32)
            sq[...] += jnp.sum(piece * piece, axis=1, keepdims=True)
            rows = pl.ds(pl.multiple_of(j * width + c * in_half, in_half), in_half)
            scaled = (piece * gain[:, rows]).astype(bf16)
            for at, w in enumerate((wq, wk, wv)):
                raw[m, :, at * inner : (at + 1) * inner] += dot_nn(scaled, w[rows, :])
            return inside

        lax.fori_loop(0, n * chunks, gathered, 0)
        inv = lax.rsqrt(sq[:, :1] / model_width + epsilon)
        inv_kept[m] = jnp.broadcast_to(inv, (seq, 128))
        proj[m] = (raw[m] * inv).astype(bf16)
        mask_row = jnp.where(tokens[pl.ds(m, 1), :] == 0, neg_fill, 0.0)
        for p in range(groups):
            cols = slice(p * 128, (p + 1) * 128)
            q = proj[m, :, p * 128 : (p + 1) * 128]
            k = proj[m, :, inner + p * 128 : inner + (p + 1) * 128]
            v = proj[m, :, 2 * inner + p * 128 : 2 * inner + (p + 1) * 128]
            scores = dot_nt(spread(q), k)
            scores = scores + bias[p * per : (p + 1) * per].reshape(per * seq, seq) + mask_row
            top = jnp.max(scores, axis=-1, keepdims=True)
            grown = jnp.exp(scores - top)
            prob = grown / jnp.sum(grown, axis=-1, keepdims=True)
            probs[m, p] = prob
            mixg[m, me, :, cols] = fold(dot_nn(prob.astype(bf16), v)).astype(bf16)
            if (p + 1) % (groups // chunks) == 0:
                c = p // (groups // chunks)

                @pl.when(sec < sections - 1)
                def _():
                    for i in range(n - 1, 0, -1):
                        unless_far(i, lambda i=i: mix_copy(m, peer(i), c).start())

        @pl.when(is_first & (m + 1 < micro))
        def _():
            send_x(m + 1)

    def project(m):
        @pl.when(sec < sections - 1)
        def _():
            acc[...] = xin[m, me].astype(f32)

            def mixed(at, inside):
                i = visit(at)
                j = peer(i)

                @pl.when(i > 0)
                def _():
                    for c in range(chunks):
                        part = mixg.at[m, j, :, mix_cols(c)]
                        remote(part, part, m_s.at[m, j, c], m_r.at[m, j, c], sec, j).wait_recv()
                        if relayed:
                            pl.when((i == n - 2) & inner_chip)(on_mix(m, j, c).start)

                rows = pl.ds(pl.multiple_of(j * inner, inner), inner)
                acc[...] += dot_nn(mixg[m, j], wo[rows, :])
                return inside

            lax.fori_loop(0, n, mixed, 0)
            share[m] = acc[...].astype(bf16)
            for c in range(chunks):
                for i in range(n - 1, -1, -1):
                    unless_far(i, lambda i=i, c=c: y_copy(m, peer(i), c).start())

    def i_copy(m, j, c):
        return remote(
            ins.at[m, j, :, in_cols(c)], ip.at[m, me, :, in_cols(c)],
            i_s.at[m, j, c], i_r.at[m, me, c], sec, j,
        )

    def r_copy(m, j):
        return remote(rads.at[m], rad.at[m, me], r_s.at[m, j], r_r.at[m, me], sec, j)

    def g_copy(m, to_sec):
        return remote(grad.at[m], gin.at[m], g_s.at[m], g_r.at[m], to_sec, me)

    def t_copy(i):
        other = member(i)
        return pltpu.make_async_remote_copy(
            src_ref=tab.at[mine], dst_ref=tab.at[mine],
            send_sem=t_s.at[other], recv_sem=t_r.at[mine],
            device_id={"section": other // dps, "dp": other % dps}, device_id_type=MESH,
        )

    def d_copy(i):
        other = (dp + i) % dps
        return pltpu.make_async_remote_copy(
            src_ref=gains.at[dp], dst_ref=gains.at[dp],
            send_sem=d_s.at[other], recv_sem=d_r.at[dp],
            device_id={"dp": other}, device_id_type=MESH,
        )

    def receive(m):
        pl.when((m == 0) & ~flips_first)(flip_all)
        g_copy(m, sec + 1).wait_recv()
        head_parts(m, gin)

    def backward(m):
        @pl.when(is_last)
        def _():
            gin[m] = cotangent[m]

        mg_ref[...] = hs[m, me].astype(f32)

        def arrived(i, inside):
            j = peer(i)

            def add():
                for c in range(chunks):
                    remote(
                        hs.at[m, j, :, mix_cols(c)], hp.at[m, j, :, mix_cols(c)],
                        h_s.at[m, j, c], h_r.at[m, j, c], sec, j,
                    ).wait_recv()
                mg_ref[...] += hp[m, j].astype(f32)

            unless_far(i, add)
            return inside

        lax.fori_loop(1, n, arrived, 0)
        inv = inv_kept[m][:, :1]
        radial = jnp.zeros((seq, 128), f32)
        for p in range(groups):
            q_cols = slice(p * 128, (p + 1) * 128)
            k_cols = slice(inner + p * 128, inner + (p + 1) * 128)
            v_cols = slice(2 * inner + p * 128, 2 * inner + (p + 1) * 128)
            q2 = spread(proj[m, :, q_cols])
            k = proj[m, :, k_cols]
            v = proj[m, :, v_cols]
            mg2 = spread(mg_ref[:, q_cols].astype(bf16))
            prob = probs[m, p]
            prob_grad = dot_nt(mg2, v)
            value_grad = dot_tn(prob.astype(bf16), mg2)
            score_grad = prob * (prob_grad - jnp.sum(prob_grad * prob, axis=-1, keepdims=True))
            wide = jnp.concatenate([score_grad, jnp.zeros_like(score_grad)], axis=1)
            for e in range(per):
                part = wide[e * seq : e * seq + 8]
                for a in range(8, seq, 8):
                    part = part + pltpu.roll(
                        wide[e * seq + a : e * seq + a + 8], (2 * seq - a) % (2 * seq), 1
                    )
                diag[p * per + e] += part
            half = score_grad.astype(bf16)
            query_grad = fold(dot_nn(half, k))
            key_grad = dot_tn(half, q2)
            for cols, part in ((q_cols, query_grad), (k_cols, key_grad), (v_cols, value_grad)):
                radial = radial + part * raw[m, :, cols]
                sgr[:, cols] = (part * inv).astype(bf16)
        rads[m] = jnp.broadcast_to(jnp.sum(radial, axis=1, keepdims=True), (seq, 128)).T[:8]
        for i in range(n - 1, 0, -1):
            r_copy(m, peer(i)).start()

        def input_part(step, inside):
            i = emit(step // chunks)
            c = step % chunks
            at = pl.ds(pl.multiple_of(peer(i) * width + c * in_half, in_half), in_half)
            part = dot_nn(sgr[:, :inner], wq_t[:, at])
            part += dot_nn(sgr[:, inner : 2 * inner], wk_t[:, at])
            part += dot_nn(sgr[:, 2 * inner :], wv_t[:, at])
            pass_on(m, i, c, in_cols(c), part, ins, ex_i, i_s, ei_r, i_copy)
            return inside

        lax.fori_loop(0, n * chunks, input_part, 0)

        @pl.when(m == micro - 1)
        def _():
            sub = lax.broadcasted_iota(jnp.int32, (8, 2 * seq), 0)
            for h in range(heads):
                part = diag[h]
                for bit in (1, 2, 4):
                    moved = pltpu.roll(part, 2 * seq - bit, 1)
                    part = jnp.where((sub // bit) % 2 == 1, moved, part)
                tab[mine, h : h + 1] = jnp.sum(part, axis=0, keepdims=True)
            for i in range(1, everyone):
                t_copy(i).start()

    def settle(m):
        inv = inv_kept[m][:, :1]
        acc[...] = ins[m, me].astype(f32)
        sq[:8, :seq] = rads[m]

        def arrived_input(i, inside):
            j = peer(i)
            remote(rads.at[m], rad.at[m, j], r_s.at[m, j], r_r.at[m, j], sec, j).wait_recv()
            sq[:8, :seq] += rad[m, j]

            def add():
                for c in range(chunks):
                    remote(
                        ins.at[m, j, :, in_cols(c)], ip.at[m, j, :, in_cols(c)],
                        i_s.at[m, j, c], i_r.at[m, j, c], sec, j,
                    ).wait_recv()
                acc[...] += ip[m, j].astype(f32)

            unless_far(i, add)
            return inside

        lax.fori_loop(1, n, arrived_input, 0)
        radial_sum = jnp.broadcast_to(sq[:1, :seq], (128, seq)).T[:, :1]
        rows_f32 = xin[m, me].astype(f32)
        normed = acc[...]
        gain_own = gain[:, pl.ds(pl.multiple_of(me * width, width), width)]
        weight = radial_sum * inv * inv * inv / model_width
        result = (gin[m].astype(f32) + normed * gain_own - weight * rows_f32).astype(bf16)
        grad[m] = result
        grads_out[0, m] = result

        @pl.when(sec > 0)
        def _():
            g_copy(m, sec - 1).start()

        gains[dp] += jnp.sum(normed * rows_f32, axis=0, keepdims=True)

    def step(t, carry):
        u = t - 2 * micro
        kind = jnp.where(u < 0, t % 2, u % 3 + 2)
        m = jnp.where(u < 0, t // 2, u // 3)
        of_last = t % 3
        kind = jnp.where(is_last, jnp.where(of_last == 0, 0, of_last + 2), kind)
        m = jnp.where(is_last, t // 3, m)
        busy = ~is_last | (t < 3 * micro)

        for at, act in enumerate((forward, project, receive, backward, settle)):
            pl.when((kind == at) & busy)(lambda act=act: act(m))

        return carry

    lax.fori_loop(0, 5 * micro, step, 0)
    for i in range(1, dps):
        d_copy(i).start()

    def finish(m, carry):
        def one(i, inside):
            j = peer(i)
            r_copy(m, j).wait_send()
            for c in range(chunks):
                h_copy(m, j, c).wait_send()
                i_copy(m, j, c).wait_send()

                @pl.when(is_first)
                def _():
                    unless_far(i, x_copy(m, j, c).wait_send)

                @pl.when(sec < sections - 1)
                def _():
                    unless_far(i, mix_copy(m, j, c).wait_send)

            return inside

        lax.fori_loop(1, n, one, 0)
        if relayed:

            for c in range(chunks):
                pl.when(inner_chip)(on_x(m, peer(n - 2), c).wait_send)
                pl.when(inner_chip & (sec < sections - 1))(on_mix(m, peer(n - 2), c).wait_send)

        @pl.when(sec > 0)
        def _():
            g_copy(m, sec - 1).wait_send()

        return carry

    lax.fori_loop(0, micro, finish, 0)

    @pl.when(sec < sections - 1)
    def _():
        def one(m, carry):
            for i in range(n):
                for c in range(chunks):
                    unless_far(i, y_copy(m, peer(i), c).wait_send)
            return carry

        lax.fori_loop(0, micro, one, 0)

    def table_wait(i, carry):
        other = member(i)
        pltpu.make_async_remote_copy(
            src_ref=tab.at[mine], dst_ref=tab.at[other],
            send_sem=t_s.at[other], recv_sem=t_r.at[other],
            device_id={"section": other // dps, "dp": other % dps}, device_id_type=MESH,
        ).wait()
        return carry

    lax.fori_loop(1, everyone, table_wait, 0)
    total = tab[0]
    for at in range(1, everyone):
        total = total + tab[at]
    last = buckets[seq - 1 : seq, :]
    place = jnp.concatenate([buckets[0:1, :], last[:, seq - 1 :], last[:, : seq - 1]], axis=1)
    summed = jnp.zeros(total.shape, f32)
    for c in range(table.shape[1]):
        part = jnp.sum(jnp.where(place == c, total, 0.0), axis=1, keepdims=True)
        summed = jnp.where(lane == c, part, summed)
    table_out[...] = summed[:heads, : table_out.shape[1]]
    for i in range(1, dps):
        other = (dp + i) % dps
        pltpu.make_async_remote_copy(
            src_ref=gains.at[dp], dst_ref=gains.at[other],
            send_sem=d_s.at[other], recv_sem=d_r.at[other],
            device_id={"dp": other}, device_id_type=MESH,
        ).wait()
    total = gains[0]
    for at in range(1, dps):
        total = total + gains[at]
    gain_out[...] = total


def hand_on(grads, gains, table, grads_out, gains_out, table_out):
    grads_out[...] = grads[...]
    gains_out[...] = gains[...]
    table_out[...] = table[...]


def per_device(
    stream, cotangent, token_ids, buckets, bias_table, gain, w_query, w_key, w_value, w_out
):
    sections = lax.axis_size("section")
    n = lax.axis_size("mp")
    dps = lax.axis_size("dp")
    micro, seq, width = stream.shape
    heads = bias_table.shape[1]
    inner = w_query.shape[2]
    head_dim = inner // heads
    groups = heads * head_dim // 128
    per = 128 // head_dim
    vmem = pl.BlockSpec(memory_space=pltpu.VMEM)
    hbm = pl.BlockSpec(memory_space=pl.ANY)
    dma = pltpu.SemaphoreType.DMA
    grads, gains, table_grad = pl.pallas_call(
        functools.partial(relay_kernel, sections, n, dps, head_dim),
        out_shape=(
            jax.ShapeDtypeStruct((1, micro, seq, width), bf16),
            jax.ShapeDtypeStruct((1, width), f32),
            jax.ShapeDtypeStruct(bias_table.shape[::-1], f32),
        ),
        in_specs=[vmem, vmem, vmem, vmem, pl.BlockSpec(memory_space=pltpu.SMEM), vmem]
        + [hbm] * 4,
        out_specs=(vmem, vmem, vmem),
        scratch_shapes=[
            pltpu.VMEM(w_query.shape[1:], bf16),
            pltpu.VMEM(w_key.shape[1:], bf16),
            pltpu.VMEM(w_value.shape[1:], bf16),
            pltpu.VMEM(w_out.shape[1:], bf16),
            pltpu.VMEM(w_query.shape[:0:-1], bf16),
            pltpu.VMEM(w_key.shape[:0:-1], bf16),
            pltpu.VMEM(w_value.shape[:0:-1], bf16),
            pltpu.VMEM(w_out.shape[:0:-1], bf16),
            pltpu.VMEM((heads, seq, seq), f32),
            pltpu.VMEM((micro, n, seq, width), bf16),
            pltpu.VMEM((micro, n, seq, inner), bf16),
            pltpu.VMEM((micro, n, seq, inner), bf16),
            pltpu.VMEM((micro, n, seq, width), bf16),
            pltpu.VMEM((micro, n, 8, seq), f32),
            pltpu.VMEM((micro, seq, width), bf16),
            pltpu.VMEM((micro, n, seq, inner), bf16),
            pltpu.VMEM((micro, n, seq, width), bf16),
            pltpu.VMEM((micro, 8, seq), f32),
            pltpu.VMEM((micro, seq, width), bf16),
            pltpu.VMEM((micro, seq, width), bf16),
            pltpu.VMEM((micro, seq, 3 * inner), f32),
            pltpu.VMEM((micro, seq, 3 * inner), bf16),
            pltpu.VMEM((micro, groups, per * seq, seq), f32),
            pltpu.VMEM((micro, seq, 128), f32),
            pltpu.VMEM((seq, width), f32),
            pltpu.VMEM((seq, inner), f32),
            pltpu.VMEM((seq, 3 * inner), bf16),
            pltpu.VMEM((seq, 128), f32),
            pltpu.VMEM((heads, 8, 2 * seq), f32),
            pltpu.VMEM((sections * dps, max(heads, 8), 2 * seq), f32),
            pltpu.VMEM((dps, 1, width), f32),
            pltpu.VMEM((micro, seq, inner), bf16),
            pltpu.VMEM((micro, seq, width), bf16),
            dma((4,)),
            dma((micro,)),
        ]
        + [dma((micro, n, 2))] * 9
        + [dma((micro, n))] * 2
        + [dma((micro,))] * 2
        + [dma((sections * dps,))] * 2
        + [dma((dps,))] * 2
        + [dma((micro, 2))] * 4,
        compiler_params=pltpu.CompilerParams(
            collective_id=0, has_side_effects=True, vmem_limit_bytes=60 * 1024 * 1024
        ),
    )(
        stream, cotangent, token_ids, buckets, bias_table.T, gain, w_query, w_key, w_value, w_out,
    )
    grads, gains, table_grad = pl.pallas_call(
        hand_on,
        out_shape=(
            jax.ShapeDtypeStruct(grads.shape, bf16),
            jax.ShapeDtypeStruct(gains.shape, f32),
            jax.ShapeDtypeStruct(table_grad.shape, f32),
        ),
        in_specs=[vmem] * 3,
        out_specs=(vmem,) * 3,
    )(grads, gains, table_grad)
    return grads, gains, table_grad.T


def solution(mesh):
    in_specs = (
        P("dp", None, "mp"),
        P("dp", None, "mp"),
        P("dp", None),
        P(),
        P(None, "mp"),
        P("section", None),
        P("section", None, "mp"),
        P("section", None, "mp"),
        P("section", None, "mp"),
        P("section", None, "mp"),
    )
    out_specs = (P("section", "dp", None, "mp"), P("section", "mp"), P(None, "mp"))
    return jax.shard_map(
        per_device, mesh=mesh, in_specs=in_specs, out_specs=out_specs, check_vma=False
    )
```

```python
import functools

import jax
import jax.numpy as jnp
from jax import lax
from jax.experimental import pallas as pl
from jax.experimental.pallas import tpu as pltpu
from jax.sharding import PartitionSpec as P

neg_fill = -1000000000.0
epsilon = 1e-06
MESH = pl.DeviceIdType.MESH
DELAY = 8000
DELAYED = 1
f32 = jnp.float32
bf16 = jnp.bfloat16


def dot_nn(a, b):
    return lax.dot_general(a, b, (((1,), (0,)), ((), ())), preferred_element_type=f32)


def dot_nt(a, b):
    return lax.dot_general(a, b, (((1,), (1,)), ((), ())), preferred_element_type=f32)


def dot_tn(a, b):
    return lax.dot_general(a, b, (((0,), (0,)), ((), ())), preferred_element_type=f32)


def relay_kernel(
    sections, n, dps, head_dim,
    stream, cotangent, tokens, buckets, table, gain, wq_hbm, wk_hbm, wv_hbm, wo_hbm,
    grads_out, gain_out, table_out,
    wq, wk, wv, wo, wq_t, wk_t, wv_t, wo_t, bias, xin, mixg, hp, ip, rad, gin, hs, ins, rads, share, grad, up, gain_own, gain_n, gains_n,
    raw, proj, probs, inv_kept, acc, mg_ref, sgr, sq, diag, tab, gains, ex_h, ex_i,
    w_sem, l_sem, x_s, y_s, x_r, m_s, m_r, h_s, h_r, i_s, i_r, r_s, r_r, b_s, b_r, u_s, u_r, q_s, q_r, e_s, t_s, t_r, d_s, d_r, fx_s, fm_s, eh_r, ei_r,
):
    micro, seq, width = stream.shape
    heads = bias.shape[0]
    inner = heads * head_dim
    per = 128 // head_dim
    groups = heads // per
    model_width = n * width
    sec = lax.axis_index("section")
    me = lax.axis_index("mp")
    dp = lax.axis_index("dp")
    everyone = sections * dps
    mine = sec * dps + dp
    turn = 1 - 2 * (me // ((n + 1) // 2))

    def peer(i):
        return (me + i * turn + n) % n

    relayed = n == 4
    chunks = 2 if relayed and inner % 256 == 0 and width % 256 == 0 else 1
    in_half, mix_half = width // chunks, inner // chunks

    def in_cols(c):
        return pl.ds(pl.multiple_of(c * in_half, in_half), in_half)

    def mix_cols(c):
        return pl.ds(pl.multiple_of(c * mix_half, mix_half), mix_half)

    def flip(src, dst):
        rows = min(256, src.shape[0])

        def one(r, carry):
            at = pl.ds(pl.multiple_of(r * rows, rows), rows)
            dst[:, at] = src[at, :].T
            return carry

        lax.fori_loop(0, src.shape[0] // rows, one, 0)

    def flip_all():
        for src, dst in ((wo, wo_t), (wq, wq_t), (wk, wk_t), (wv, wv_t)):
            flip(src, dst)

    flips_first = sec * 2 >= sections
    inner_chip = (me % (n - 1)) != 0 if relayed else True

    def visit(at):
        return jnp.where(at == 1, 2, jnp.where(at == 2, 1, at)) if relayed else at

    def unless_far(i, act):
        if relayed:
            pl.when((i < n - 1) | inner_chip)(act)
        else:
            act()

    def remote(src, dst, ssem, rsem, to_sec, to_mp):
        return pltpu.make_async_remote_copy(
            src_ref=src, dst_ref=dst, send_sem=ssem, recv_sem=rsem,
            device_id={"section": to_sec, "mp": to_mp}, device_id_type=MESH,
        )

    loads = [
        pltpu.make_async_copy(src, dst, w_sem.at[at])
        for at, (src, dst) in enumerate(
            ((wq_hbm.at[0], wq), (wk_hbm.at[0], wk), (wv_hbm.at[0], wv), (wo_hbm.at[0], wo))
        )
    ]
    for load in loads:
        load.start()

    barrier = pltpu.get_barrier_semaphore()
    is_first = sec == 0
    is_last = sec == sections - 1
    for i in range(1, n):
        pl.semaphore_signal(
            barrier, inc=1, device_id={"section": sec, "mp": peer(i)}, device_id_type=MESH
        )

    @pl.when(sec > 0)
    def _():
        for j in range(n):
            pl.semaphore_signal(
                barrier, inc=1, device_id={"section": sec - 1, "mp": j}, device_id_type=MESH
            )

    @pl.when(sec < sections - 1)
    def _():
        for j in range(n):
            pl.semaphore_signal(
                barrier, inc=1, device_id={"section": sec + 1, "mp": j}, device_id_type=MESH
            )

    def member(i):
        return (mine + i) % everyone

    for i in range(1, everyone):
        other = member(i)
        pl.semaphore_signal(
            barrier, inc=1, device_id={"section": other // dps, "dp": other % dps},
            device_id_type=MESH,
        )

    greeters = n - 1 + everyone - 1 + n * jnp.minimum(sec, 1) + n * jnp.minimum(sections - 1 - sec, 1)
    pl.semaphore_wait(barrier, greeters)

    above = jnp.maximum(sec - 1, 0)
    bank = jnp.minimum(sec, 1)

    def q_copy():
        return remote(gain_own, gain_n, q_s.at[0], q_r.at[0], above, me)

    gain_own[...] = gain[:, pl.ds(pl.multiple_of(me * width, width), width)]
    pl.when(sec > 0)(lambda: q_copy().start())
    gains_n[...] = jnp.zeros(gains_n.shape, f32)

    @pl.when(sec == sections - 2)
    def _():
        up[...] = cotangent[...]

    def x_copy(m, j, c):
        return remote(
            stream.at[m, :, in_cols(c)], xin.at[m, me, :, in_cols(c)],
            x_s.at[m, j, c], x_r.at[m, me, c], sec, j,
        )

    def y_copy(m, j, c):
        return remote(
            share.at[m, :, in_cols(c)], xin.at[m, me, :, in_cols(c)],
            y_s.at[m, j, c], x_r.at[m, me, c], sec + 1, j,
        )

    def send_x(m):
        pltpu.make_async_copy(stream.at[m], xin.at[m, me], l_sem.at[m]).start()
        for c in range(chunks):
            for i in range(n - 1, 0, -1):
                unless_far(i, lambda i=i, c=c: x_copy(m, peer(i), c).start())

    @pl.when(is_first)
    def _():
        @pl.when(dp % 2 == DELAYED)
        def _():
            pl.delay(DELAY)

        send_x(0)

    def head_bias(h, carry):
        value = jnp.zeros((seq, seq), f32)
        held = buckets[...]
        for c in range(table.shape[1]):
            value = jnp.where(held == c, table[h, c], value)
        bias[h] = value
        return carry

    lax.fori_loop(0, heads, head_bias, 0)
    tab[mine] = jnp.zeros(tab.shape[1:], f32)
    diag[...] = jnp.zeros(diag.shape, f32)
    gains[dp] = jnp.zeros(gains.shape[1:], f32)
    for load in loads:
        load.wait()
    pl.when(flips_first)(flip_all)

    def h_copy(m, j, c):
        return remote(
            hs.at[m, j, :, mix_cols(c)], hp.at[m, me, :, mix_cols(c)],
            h_s.at[m, j, c], h_r.at[m, me, c], sec, j,
        )

    def emit(at):
        return jnp.where(at == 0, 3, jnp.where(at == 3, 2, 2 - at)) if relayed else n - 1 - at

    def pass_on(m, i, c, cols, part, own, extra, own_sem, extra_sem, copy, lifted):
        j = peer(i)
        own[m, j, :, cols] = part.astype(bf16)
        if not relayed:
            pl.when((i > 0) | lifted)(lambda: copy(m, j, c).start())
            return

        def hand_over():
            return remote(
                own.at[m, j, :, cols], extra.at[m, :, cols],
                own_sem.at[m, j, c], extra_sem.at[m, c], sec, peer(1),
            )

        @pl.when((i == n - 2) & inner_chip)
        def _():
            hand_over().wait_recv()
            own[m, j, :, cols] = (part + extra[m, :, cols].astype(f32)).astype(bf16)

        @pl.when(((i > 0) | lifted) & ((i < n - 1) | inner_chip))
        def _():
            copy(m, j, c).start()

        @pl.when((i == n - 1) & ((me % (n - 1)) == 0))
        def _():
            hand_over().start()

    def head_parts(m, upstream):
        def one(step, carry):
            i = emit(step)
            j = peer(i)
            cols = pl.ds(pl.multiple_of(j * inner, inner), inner)
            part = dot_nn(upstream[m], wo_t[:, cols])
            for c in range(chunks):
                at = slice(c * mix_half, (c + 1) * mix_half)
                pass_on(m, i, c, at, part[:, at], hs, ex_h, h_s, eh_r, h_copy, False)
            return carry

        lax.fori_loop(0, n, one, 0)

    @pl.when(is_last)
    def _():
        def one(m, carry):
            head_parts(m, cotangent)
            return carry

        lax.fori_loop(0, micro, one, 0)

    lane = lax.broadcasted_iota(jnp.int32, (1, 128), 1)
    picks = [
        jnp.where((lane // head_dim) == e, 1.0, 0.0).astype(f32) for e in range(per)
    ]
    picks_half = [pick.astype(bf16) for pick in picks]

    def spread(block):
        return jnp.concatenate([block * pick for pick in picks_half], axis=0)

    def fold(block):
        total = block[:seq] * picks[0]
        for e in range(1, per):
            total = total + block[e * seq : (e + 1) * seq] * picks[e]
        return total

    def mix_copy(m, j, c):
        part = mixg.at[m, me, :, mix_cols(c)]
        return remote(part, part, m_s.at[m, j, c], m_r.at[m, me, c], sec, j)

    def on_x(m, j, c):
        part = xin.at[m, j, :, in_cols(c)]
        return remote(part, part, fx_s.at[m, c], x_r.at[m, j, c], sec, peer(n - 1))

    def on_mix(m, j, c):
        part = mixg.at[m, j, :, mix_cols(c)]
        return remote(part, part, fm_s.at[m, c], m_r.at[m, j, c], sec, peer(n - 1))

    def forward(m):
        @pl.when(is_first)
        def _():
            pltpu.make_async_copy(stream.at[m], xin.at[m, me], l_sem.at[m]).wait()

        raw[m] = jnp.zeros(raw.shape[1:], f32)
        sq[...] = jnp.zeros(sq.shape, f32)

        def gathered(step, inside):
            i = visit(step // chunks)
            j = peer(i)
            c = step % chunks

            @pl.when((sec > 0) | (i > 0))
            def _():
                remote(
                    share.at[m, :, in_cols(c)], xin.at[m, j, :, in_cols(c)],
                    x_s.at[m, j, c], x_r.at[m, j, c], sec, j,
                ).wait_recv()

            if relayed:

                @pl.when((i == n - 2) & inner_chip)
                def _():
                    on_x(m, j, c).start()

            piece = xin[m, j, :, in_cols(c)].astype(f32)
            sq[...] += jnp.sum(piece * piece, axis=1, keepdims=True)
            rows = pl.ds(pl.multiple_of(j * width + c * in_half, in_half), in_half)
            scaled = (piece * gain[:, rows]).astype(bf16)
            for at, w in enumerate((wq, wk, wv)):
                raw[m, :, at * inner : (at + 1) * inner] += dot_nn(scaled, w[rows, :])
            return inside

        lax.fori_loop(0, n * chunks, gathered, 0)
        inv = lax.rsqrt(sq[:, :1] / model_width + epsilon)
        inv_kept[m] = jnp.broadcast_to(inv, (seq, 128))
        proj[m] = (raw[m] * inv).astype(bf16)
        mask_row = jnp.where(tokens[pl.ds(m, 1), :] == 0, neg_fill, 0.0)
        for p in range(groups):
            cols = slice(p * 128, (p + 1) * 128)
            q = proj[m, :, p * 128 : (p + 1) * 128]
            k = proj[m, :, inner + p * 128 : inner + (p + 1) * 128]
            v = proj[m, :, 2 * inner + p * 128 : 2 * inner + (p + 1) * 128]
            scores = dot_nt(spread(q), k)
            scores = scores + bias[p * per : (p + 1) * per].reshape(per * seq, seq) + mask_row
            top = jnp.max(scores, axis=-1, keepdims=True)
            grown = jnp.exp(scores - top)
            prob = grown / jnp.sum(grown, axis=-1, keepdims=True)
            probs[m, p] = prob
            mixg[m, me, :, cols] = fold(dot_nn(prob.astype(bf16), v)).astype(bf16)
            if (p + 1) % (groups // chunks) == 0:
                c = p // (groups // chunks)

                @pl.when(sec < sections - 1)
                def _():
                    for i in range(n - 1, 0, -1):
                        unless_far(i, lambda i=i: mix_copy(m, peer(i), c).start())

        @pl.when(is_first & (m + 1 < micro))
        def _():
            send_x(m + 1)

    def project(m):
        @pl.when(sec < sections - 1)
        def _():
            acc[...] = xin[m, me].astype(f32)

            def mixed(at, inside):
                i = visit(at)
                j = peer(i)

                @pl.when(i > 0)
                def _():
                    for c in range(chunks):
                        part = mixg.at[m, j, :, mix_cols(c)]
                        remote(part, part, m_s.at[m, j, c], m_r.at[m, j, c], sec, j).wait_recv()
                        if relayed:
                            pl.when((i == n - 2) & inner_chip)(on_mix(m, j, c).start)

                rows = pl.ds(pl.multiple_of(j * inner, inner), inner)
                acc[...] += dot_nn(mixg[m, j], wo[rows, :])
                return inside

            lax.fori_loop(0, n, mixed, 0)
            share[m] = acc[...].astype(bf16)
            for c in range(chunks):
                for i in range(n - 1, -1, -1):
                    unless_far(i, lambda i=i, c=c: y_copy(m, peer(i), c).start())

    def i_copy(m, j, c):
        return remote(
            ins.at[m, j, :, in_cols(c)], ip.at[bank, m, me, :, in_cols(c)],
            i_s.at[m, j, c], i_r.at[bank, m, me, c], above, j,
        )

    def r_copy(m, j):
        return remote(
            rads.at[m], rad.at[bank, m, me], r_s.at[m, j], r_r.at[bank, m, me], above, j
        )

    def back_copy(m):
        return remote(gin.at[m], grad.at[m], b_s.at[m], b_r.at[m], sec + 1, me)

    def up_copy(m):
        return remote(gin.at[m], up.at[m], u_s.at[m], u_r.at[m], above, me)

    def t_copy(i):
        other = member(i)
        return pltpu.make_async_remote_copy(
            src_ref=tab.at[mine], dst_ref=tab.at[mine],
            send_sem=t_s.at[other], recv_sem=t_r.at[mine],
            device_id={"section": other // dps, "dp": other % dps}, device_id_type=MESH,
        )

    def d_copy(i):
        other = (dp + i) % dps
        return pltpu.make_async_remote_copy(
            src_ref=gains.at[dp], dst_ref=gains.at[dp],
            send_sem=d_s.at[other], recv_sem=d_r.at[dp],
            device_id={"dp": other}, device_id_type=MESH,
        )

    def e_copy(other):
        return pltpu.make_async_remote_copy(
            src_ref=gains_n, dst_ref=gains.at[dp], send_sem=e_s.at[other], recv_sem=d_r.at[dp],
            device_id={"section": sec + 1, "dp": other}, device_id_type=MESH,
        )

    def combine(m, deep, upstream, rows, gain_part):
        if deep:
            acc[...] = jnp.zeros(acc.shape, f32)
            sq[:8, :seq] = jnp.zeros((8, seq), f32)
        else:
            acc[...] = ins[m, me].astype(f32)
            sq[:8, :seq] = rads[m]

        def arrived_input(i, inside):
            j = peer(i)
            remote(
                rads.at[m], rad.at[deep, m, j], r_s.at[m, j], r_r.at[deep, m, j], sec, j
            ).wait_recv()
            sq[:8, :seq] += rad[deep, m, j]

            def add():
                for c in range(chunks):
                    remote(
                        ins.at[m, j, :, in_cols(c)], ip.at[deep, m, j, :, in_cols(c)],
                        i_s.at[m, j, c], i_r.at[deep, m, j, c], sec, j,
                    ).wait_recv()
                acc[...] += ip[deep, m, j].astype(f32)

            unless_far(i, add)
            return inside

        lax.fori_loop(1 - deep, n, arrived_input, 0)
        inv = rad[1, m, me, 1:2, :] if deep else rads[m, 1:2, :]
        weight = sq[:1, :seq] * inv * inv * inv / model_width
        weight = jnp.broadcast_to(weight, (128, seq)).T[:, :1]
        rows_f32 = rows.astype(f32)
        normed = acc[...]
        result = (upstream.astype(f32) + normed * gain_part - weight * rows_f32).astype(bf16)
        return result, jnp.sum(normed * rows_f32, axis=0, keepdims=True)

    def receive(m):
        @pl.when(m == 0)
        def _():
            pl.when(~flips_first)(flip_all)
            remote(gain_own, gain_n, q_s.at[0], q_r.at[0], sec, me).wait_recv()

        @pl.when(sec < sections - 2)
        def _():
            remote(gin.at[m], up.at[m], u_s.at[m], u_r.at[m], sec, me).wait_recv()

        result, part = combine(m, 1, up[m], share[m], gain_n[...])
        gin[m] = result
        head_parts(m, gin)
        back_copy(m).start()
        pl.when(sec > 0)(lambda: up_copy(m).start())
        gains_n[...] += part

        @pl.when(m == micro - 1)
        def _():
            for other in range(dps):
                e_copy(other).start()

    def backward(m):
        mg_ref[...] = hs[m, me].astype(f32)

        def arrived(i, inside):
            j = peer(i)

            def add():
                for c in range(chunks):
                    remote(
                        hs.at[m, j, :, mix_cols(c)], hp.at[m, j, :, mix_cols(c)],
                        h_s.at[m, j, c], h_r.at[m, j, c], sec, j,
                    ).wait_recv()
                mg_ref[...] += hp[m, j].astype(f32)

            unless_far(i, add)
            return inside

        lax.fori_loop(1, n, arrived, 0)
        inv = inv_kept[m][:, :1]
        radial = jnp.zeros((seq, 128), f32)
        for p in range(groups):
            q_cols = slice(p * 128, (p + 1) * 128)
            k_cols = slice(inner + p * 128, inner + (p + 1) * 128)
            v_cols = slice(2 * inner + p * 128, 2 * inner + (p + 1) * 128)
            q2 = spread(proj[m, :, q_cols])
            k = proj[m, :, k_cols]
            v = proj[m, :, v_cols]
            mg2 = spread(mg_ref[:, q_cols].astype(bf16))
            prob = probs[m, p]
            prob_grad = dot_nt(mg2, v)
            value_grad = dot_tn(prob.astype(bf16), mg2)
            score_grad = prob * (prob_grad - jnp.sum(prob_grad * prob, axis=-1, keepdims=True))
            wide = jnp.concatenate([score_grad, jnp.zeros_like(score_grad)], axis=1)
            for e in range(per):
                part = wide[e * seq : e * seq + 8]
                for a in range(8, seq, 8):
                    part = part + pltpu.roll(
                        wide[e * seq + a : e * seq + a + 8], (2 * seq - a) % (2 * seq), 1
                    )
                diag[p * per + e] += part
            half = score_grad.astype(bf16)
            query_grad = fold(dot_nn(half, k))
            key_grad = dot_tn(half, q2)
            for cols, part in ((q_cols, query_grad), (k_cols, key_grad), (v_cols, value_grad)):
                radial = radial + part * raw[m, :, cols]
                sgr[:, cols] = (part * inv).astype(bf16)
        rads[m] = jnp.where(lane == 0, jnp.sum(radial, axis=1, keepdims=True), inv).T[:8]
        for i in range(n - 1, 0, -1):
            r_copy(m, peer(i)).start()
        pl.when(sec > 0)(lambda: r_copy(m, me).start())

        def input_part(step, inside):
            i = emit(step // chunks)
            c = step % chunks
            at = pl.ds(pl.multiple_of(peer(i) * width + c * in_half, in_half), in_half)
            part = dot_nn(sgr[:, :inner], wq_t[:, at])
            part += dot_nn(sgr[:, inner : 2 * inner], wk_t[:, at])
            part += dot_nn(sgr[:, 2 * inner :], wv_t[:, at])
            pass_on(m, i, c, in_cols(c), part, ins, ex_i, i_s, ei_r, i_copy, sec > 0)
            return inside

        lax.fori_loop(0, n * chunks, input_part, 0)

        @pl.when(m == micro - 1)
        def _():
            sub = lax.broadcasted_iota(jnp.int32, (8, 2 * seq), 0)
            for h in range(heads):
                part = diag[h]
                for bit in (1, 2, 4):
                    moved = pltpu.roll(part, 2 * seq - bit, 1)
                    part = jnp.where((sub // bit) % 2 == 1, moved, part)
                tab[mine, h : h + 1] = jnp.sum(part, axis=0, keepdims=True)
            for i in range(1, everyone):
                t_copy(i).start()

    def settle(m):
        result, part = combine(m, 0, gin[m], xin[m, me], gain_own[...])
        grads_out[0, m] = result
        gains[dp] += part

    def step(t, carry):
        u = t - 2 * micro
        v = t - 4 * micro
        kind = jnp.where(u < 0, t % 2, jnp.where(v < 0, u % 2 + 2, 4))
        m = jnp.where(u < 0, t // 2, jnp.where(v < 0, u // 2, v))
        kind = jnp.where(is_last, t % 2 * 3, kind)
        m = jnp.where(is_last, t // 2, m)
        busy = (t < 4 * micro) & (~is_last | (t < 2 * micro)) | is_first

        for at, act in enumerate((forward, project, receive, backward, settle)):
            pl.when((kind == at) & busy)(lambda act=act: act(m))

        return carry

    lax.fori_loop(0, 5 * micro, step, 0)

    @pl.when(is_first)
    def _():
        for i in range(1, dps):
            d_copy(i).start()

    @pl.when(sec > 0)
    def _():
        q_copy().wait_send()
        for m in range(micro):
            remote(gin.at[m], grad.at[m], b_s.at[m], b_r.at[m], sec, me).wait_recv()
            grads_out[0, m] = grad[m]
            r_copy(m, me).wait_send()
            for c in range(chunks):
                i_copy(m, me, c).wait_send()

    @pl.when(sec < sections - 1)
    def _():
        for m in range(micro):
            back_copy(m).wait_send()
            pl.when(sec > 0)(up_copy(m).wait_send)
        for other in range(dps):
            e_copy(other).wait_send()

    def finish(m, carry):
        def one(i, inside):
            j = peer(i)
            r_copy(m, j).wait_send()
            for c in range(chunks):
                h_copy(m, j, c).wait_send()
                i_copy(m, j, c).wait_send()

                @pl.when(is_first)
                def _():
                    unless_far(i, x_copy(m, j, c).wait_send)

                @pl.when(sec < sections - 1)
                def _():
                    unless_far(i, mix_copy(m, j, c).wait_send)

            return inside

        lax.fori_loop(1, n, one, 0)
        if relayed:

            for c in range(chunks):
                pl.when(inner_chip)(on_x(m, peer(n - 2), c).wait_send)
                pl.when(inner_chip & (sec < sections - 1))(on_mix(m, peer(n - 2), c).wait_send)

        return carry

    lax.fori_loop(0, micro, finish, 0)

    @pl.when(sec < sections - 1)
    def _():
        def one(m, carry):
            for i in range(n):
                for c in range(chunks):
                    unless_far(i, y_copy(m, peer(i), c).wait_send)
            return carry

        lax.fori_loop(0, micro, one, 0)

    def table_wait(i, carry):
        other = member(i)
        pltpu.make_async_remote_copy(
            src_ref=tab.at[mine], dst_ref=tab.at[other],
            send_sem=t_s.at[other], recv_sem=t_r.at[other],
            device_id={"section": other // dps, "dp": other % dps}, device_id_type=MESH,
        ).wait()
        return carry

    lax.fori_loop(1, everyone, table_wait, 0)
    total = tab[0]
    for at in range(1, everyone):
        total = total + tab[at]
    last = buckets[seq - 1 : seq, :]
    place = jnp.concatenate([buckets[0:1, :], last[:, seq - 1 :], last[:, : seq - 1]], axis=1)
    summed = jnp.zeros(total.shape, f32)
    for c in range(table.shape[1]):
        part = jnp.sum(jnp.where(place == c, total, 0.0), axis=1, keepdims=True)
        summed = jnp.where(lane == c, part, summed)
    table_out[...] = summed[:heads, : table_out.shape[1]]
    def gain_in(other):
        return pltpu.make_async_remote_copy(
            src_ref=gains.at[dp], dst_ref=gains.at[other],
            send_sem=d_s.at[other], recv_sem=d_r.at[other],
            device_id={"dp": other}, device_id_type=MESH,
        )

    for i in range(1, dps):
        other = (dp + i) % dps
        gain_in(other).wait_recv()
        pl.when(is_first)(gain_in(other).wait_send)
    pl.when(sec > 0)(gain_in(dp).wait_recv)
    total = gains[0]
    for at in range(1, dps):
        total = total + gains[at]
    gain_out[...] = total


def hand_on(grads, gains, table, grads_out, gains_out, table_out):
    grads_out[...] = grads[...]
    gains_out[...] = gains[...]
    table_out[...] = table[...]


def per_device(
    stream, cotangent, token_ids, buckets, bias_table, gain, w_query, w_key, w_value, w_out
):
    sections = lax.axis_size("section")
    n = lax.axis_size("mp")
    dps = lax.axis_size("dp")
    micro, seq, width = stream.shape
    heads = bias_table.shape[1]
    inner = w_query.shape[2]
    head_dim = inner // heads
    groups = heads * head_dim // 128
    per = 128 // head_dim
    vmem = pl.BlockSpec(memory_space=pltpu.VMEM)
    hbm = pl.BlockSpec(memory_space=pl.ANY)
    dma = pltpu.SemaphoreType.DMA
    grads, gains, table_grad = pl.pallas_call(
        functools.partial(relay_kernel, sections, n, dps, head_dim),
        out_shape=(
            jax.ShapeDtypeStruct((1, micro, seq, width), bf16),
            jax.ShapeDtypeStruct((1, width), f32),
            jax.ShapeDtypeStruct(bias_table.shape[::-1], f32),
        ),
        in_specs=[vmem, vmem, vmem, vmem, pl.BlockSpec(memory_space=pltpu.SMEM), vmem]
        + [hbm] * 4,
        out_specs=(vmem, vmem, vmem),
        scratch_shapes=[
            pltpu.VMEM(w_query.shape[1:], bf16),
            pltpu.VMEM(w_key.shape[1:], bf16),
            pltpu.VMEM(w_value.shape[1:], bf16),
            pltpu.VMEM(w_out.shape[1:], bf16),
            pltpu.VMEM(w_query.shape[:0:-1], bf16),
            pltpu.VMEM(w_key.shape[:0:-1], bf16),
            pltpu.VMEM(w_value.shape[:0:-1], bf16),
            pltpu.VMEM(w_out.shape[:0:-1], bf16),
            pltpu.VMEM((heads, seq, seq), f32),
            pltpu.VMEM((micro, n, seq, width), bf16),
            pltpu.VMEM((micro, n, seq, inner), bf16),
            pltpu.VMEM((micro, n, seq, inner), bf16),
            pltpu.VMEM((2, micro, n, seq, width), bf16),
            pltpu.VMEM((2, micro, n, 8, seq), f32),
            pltpu.VMEM((micro, seq, width), bf16),
            pltpu.VMEM((micro, n, seq, inner), bf16),
            pltpu.VMEM((micro, n, seq, width), bf16),
            pltpu.VMEM((micro, 8, seq), f32),
            pltpu.VMEM((micro, seq, width), bf16),
            pltpu.VMEM((micro, seq, width), bf16),
            pltpu.VMEM((micro, seq, width), bf16),
            pltpu.VMEM((1, width), f32),
            pltpu.VMEM((1, width), f32),
            pltpu.VMEM((1, width), f32),
            pltpu.VMEM((micro, seq, 3 * inner), f32),
            pltpu.VMEM((micro, seq, 3 * inner), bf16),
            pltpu.VMEM((micro, groups, per * seq, seq), f32),
            pltpu.VMEM((micro, seq, 128), f32),
            pltpu.VMEM((seq, width), f32),
            pltpu.VMEM((seq, inner), f32),
            pltpu.VMEM((seq, 3 * inner), bf16),
            pltpu.VMEM((seq, 128), f32),
            pltpu.VMEM((heads, 8, 2 * seq), f32),
            pltpu.VMEM((sections * dps, max(heads, 8), 2 * seq), f32),
            pltpu.VMEM((dps, 1, width), f32),
            pltpu.VMEM((micro, seq, inner), bf16),
            pltpu.VMEM((micro, seq, width), bf16),
            dma((4,)),
            dma((micro,)),
        ]
        + [dma((micro, n, 2))] * 8
        + [dma((2, micro, n, 2)), dma((micro, n)), dma((2, micro, n))]
        + [dma((micro,))] * 4
        + [dma((1,))] * 2
        + [dma((dps,))]
        + [dma((sections * dps,))] * 2
        + [dma((dps,))] * 2
        + [dma((micro, 2))] * 4,
        compiler_params=pltpu.CompilerParams(
            collective_id=0, has_side_effects=True, vmem_limit_bytes=60 * 1024 * 1024
        ),
    )(
        stream, cotangent, token_ids, buckets, bias_table.T, gain, w_query, w_key, w_value, w_out,
    )
    grads, gains, table_grad = pl.pallas_call(
        hand_on,
        out_shape=(
            jax.ShapeDtypeStruct(grads.shape, bf16),
            jax.ShapeDtypeStruct(gains.shape, f32),
            jax.ShapeDtypeStruct(table_grad.shape, f32),
        ),
        in_specs=[vmem] * 3,
        out_specs=(vmem,) * 3,
    )(grads, gains, table_grad)
    return grads, gains, table_grad.T


def solution(mesh):
    in_specs = (
        P("dp", None, "mp"),
        P("dp", None, "mp"),
        P("dp", None),
        P(),
        P(None, "mp"),
        P("section", None),
        P("section", None, "mp"),
        P("section", None, "mp"),
        P("section", None, "mp"),
        P("section", None, "mp"),
    )
    out_specs = (P("section", "dp", None, "mp"), P("section", "mp"), P(None, "mp"))
    return jax.shard_map(
        per_device, mesh=mesh, in_specs=in_specs, out_specs=out_specs, check_vma=False
    )
```

```python
import functools

import jax
import jax.numpy as jnp
from jax import lax
from jax.experimental import pallas as pl
from jax.experimental.pallas import tpu as pltpu
from jax.sharding import PartitionSpec as P

neg_fill = -1000000000.0
epsilon = 1e-06
MESH = pl.DeviceIdType.MESH
DELAY = 12000
DELAYED = 1
EARLY = True
CHUNKS = 4
TOKEN = 0
f32 = jnp.float32
bf16 = jnp.bfloat16


def dot_nn(a, b):
    return lax.dot_general(a, b, (((1,), (0,)), ((), ())), preferred_element_type=f32)


def dot_nt(a, b):
    return lax.dot_general(a, b, (((1,), (1,)), ((), ())), preferred_element_type=f32)


def dot_tn(a, b):
    return lax.dot_general(a, b, (((0,), (0,)), ((), ())), preferred_element_type=f32)


def relay_kernel(
    sections, n, dps, head_dim,
    stream, cotangent, tokens, buckets, table, gain, wq_hbm, wk_hbm, wv_hbm, wo_hbm,
    grads_out, gain_out, table_out,
    wq, wk, wv, wo, wq_t, wk_t, wv_t, wo_t, bias, xin, mixg, hp, ip, rad, gin, hs, ins, rads, share, grad, up, gain_own, gain_n, gains_n,
    raw, proj, probs, inv_kept, acc, mg_ref, sgr, sq, diag, tab, gains, ex_h, ex_i,
    w_sem, l_sem, x_s, y_s, x_r, m_s, m_r, h_s, h_r, i_s, i_r, r_s, r_r, b_s, b_r, u_s, u_r, q_s, q_r, e_s, t_s, t_r, d_s, d_r, fx_s, fm_s, eh_r, ei_r, tok,
):
    micro, seq, width = stream.shape
    heads = bias.shape[0]
    inner = heads * head_dim
    per = 128 // head_dim
    groups = heads // per
    model_width = n * width
    sec = lax.axis_index("section")
    me = lax.axis_index("mp")
    dp = lax.axis_index("dp")
    everyone = sections * dps
    mine = sec * dps + dp
    turn = 1 - 2 * (me // ((n + 1) // 2))

    def peer(i):
        return (me + i * turn + n) % n

    relayed = n == 4
    chunks = CHUNKS if relayed and inner % 512 == 0 and width % 512 == 0 else 1
    in_half, mix_half = width // chunks, inner // chunks

    def in_cols(c):
        return pl.ds(pl.multiple_of(c * in_half, in_half), in_half)

    def mix_cols(c):
        return pl.ds(pl.multiple_of(c * mix_half, mix_half), mix_half)

    def flip(src, dst):
        rows = min(256, src.shape[0])

        def one(r, carry):
            at = pl.ds(pl.multiple_of(r * rows, rows), rows)
            dst[:, at] = src[at, :].T
            return carry

        lax.fori_loop(0, src.shape[0] // rows, one, 0)

    def flip_all():
        for src, dst in ((wo, wo_t), (wq, wq_t), (wk, wk_t), (wv, wv_t)):
            flip(src, dst)

    flips_first = sec * 2 >= sections
    inner_chip = (me % (n - 1)) != 0 if relayed else True

    def visit(at):
        return jnp.where(at == 1, 2, jnp.where(at == 2, 1, at)) if relayed else at

    def unless_far(i, act):
        if relayed:
            pl.when((i < n - 1) | inner_chip)(act)
        else:
            act()

    def remote(src, dst, ssem, rsem, to_sec, to_mp):
        return pltpu.make_async_remote_copy(
            src_ref=src, dst_ref=dst, send_sem=ssem, recv_sem=rsem,
            device_id={"section": to_sec, "mp": to_mp}, device_id_type=MESH,
        )

    loads = [
        pltpu.make_async_copy(src, dst, w_sem.at[at])
        for at, (src, dst) in enumerate(
            ((wq_hbm.at[0], wq), (wk_hbm.at[0], wk), (wv_hbm.at[0], wv), (wo_hbm.at[0], wo))
        )
    ]
    for load in loads:
        load.start()

    barrier = pltpu.get_barrier_semaphore()
    is_first = sec == 0
    is_last = sec == sections - 1
    for i in range(1, n):
        pl.semaphore_signal(
            barrier, inc=1, device_id={"section": sec, "mp": peer(i)}, device_id_type=MESH
        )

    @pl.when(sec > 0)
    def _():
        for j in range(n):
            pl.semaphore_signal(
                barrier, inc=1, device_id={"section": sec - 1, "mp": j}, device_id_type=MESH
            )

    @pl.when(sec < sections - 1)
    def _():
        for j in range(n):
            pl.semaphore_signal(
                barrier, inc=1, device_id={"section": sec + 1, "mp": j}, device_id_type=MESH
            )

    def member(i):
        return (mine + i) % everyone

    for i in range(1, everyone):
        other = member(i)
        pl.semaphore_signal(
            barrier, inc=1, device_id={"section": other // dps, "dp": other % dps},
            device_id_type=MESH,
        )

    greeters = n - 1 + everyone - 1 + n * jnp.minimum(sec, 1) + n * jnp.minimum(sections - 1 - sec, 1)
    pl.semaphore_wait(barrier, greeters)

    above = jnp.maximum(sec - 1, 0)
    bank = jnp.minimum(sec, 1)

    def q_copy():
        return remote(gain_own, gain_n, q_s.at[0], q_r.at[0], above, me)

    gain_own[...] = gain[:, pl.ds(pl.multiple_of(me * width, width), width)]
    pl.when(sec > 0)(lambda: q_copy().start())
    gains_n[...] = jnp.zeros(gains_n.shape, f32)

    @pl.when(sec == sections - 2)
    def _():
        up[...] = cotangent[...]

    def x_copy(m, j, c):
        return remote(
            stream.at[m, :, in_cols(c)], xin.at[m, me, :, in_cols(c)],
            x_s.at[m, j, c], x_r.at[m, me, c], sec, j,
        )

    def y_copy(m, j, c):
        return remote(
            share.at[m, :, in_cols(c)], xin.at[m, me, :, in_cols(c)],
            y_s.at[m, j, c], x_r.at[m, me, c], sec + 1, j,
        )

    late_x = dp % 2 == 1

    def send_x(m):
        pltpu.make_async_copy(stream.at[m], xin.at[m, me], l_sem.at[m]).start()
        for c in range(chunks):
            for i in range(n - 1, 0, -1):
                unless_far(i, lambda i=i, c=c: x_copy(m, peer(i), c).start())

    @pl.when(is_first)
    def _():
        @pl.when(dp % 2 == DELAYED)
        def _():
            pl.delay(DELAY)

        send_x(0)
        if EARLY:
            for m in range(1, micro):
                pl.when(dp % 2 == 0)(functools.partial(send_x, m))

    def head_bias(h, carry):
        value = jnp.zeros((seq, seq), f32)
        held = buckets[...]
        for c in range(table.shape[1]):
            value = jnp.where(held == c, table[h, c], value)
        bias[h] = value
        return carry

    lax.fori_loop(0, heads, head_bias, 0)
    tab[mine] = jnp.zeros(tab.shape[1:], f32)
    diag[...] = jnp.zeros(diag.shape, f32)
    gains[dp] = jnp.zeros(gains.shape[1:], f32)
    for load in loads:
        load.wait()
    pl.when(flips_first)(flip_all)

    def h_copy(m, j, c):
        return remote(
            hs.at[m, j, :, mix_cols(c)], hp.at[m, me, :, mix_cols(c)],
            h_s.at[m, j, c], h_r.at[m, me, c], sec, j,
        )

    def emit(at):
        return jnp.where(at == 0, 3, jnp.where(at == 3, 2, 2 - at)) if relayed else n - 1 - at

    def pass_on(m, i, c, cols, part, own, extra, own_sem, extra_sem, copy, lifted):
        j = peer(i)
        own[m, j, :, cols] = part.astype(bf16)
        if not relayed:
            pl.when((i > 0) | lifted)(lambda: copy(m, j, c).start())
            return

        def hand_over():
            return remote(
                own.at[m, j, :, cols], extra.at[m, :, cols],
                own_sem.at[m, j, c], extra_sem.at[m, c], sec, peer(1),
            )

        @pl.when((i == n - 2) & inner_chip)
        def _():
            hand_over().wait_recv()
            own[m, j, :, cols] = (part + extra[m, :, cols].astype(f32)).astype(bf16)

        @pl.when(((i > 0) | lifted) & ((i < n - 1) | inner_chip))
        def _():
            copy(m, j, c).start()

        @pl.when((i == n - 1) & ((me % (n - 1)) == 0))
        def _():
            hand_over().start()

    def head_parts(m, upstream):
        def one(step, carry):
            i = emit(step)
            j = peer(i)
            cols = pl.ds(pl.multiple_of(j * inner, inner), inner)
            part = dot_nn(upstream[m], wo_t[:, cols])
            for c in range(chunks):
                at = slice(c * mix_half, (c + 1) * mix_half)
                pass_on(m, i, c, at, part[:, at], hs, ex_h, h_s, eh_r, h_copy, False)
            return carry

        lax.fori_loop(0, n, one, 0)

    @pl.when(is_last)
    def _():
        def one(m, carry):
            head_parts(m, cotangent)
            return carry

        lax.fori_loop(0, micro, one, 0)

    lane = lax.broadcasted_iota(jnp.int32, (1, 128), 1)
    picks = [
        jnp.where((lane // head_dim) == e, 1.0, 0.0).astype(f32) for e in range(per)
    ]
    picks_half = [pick.astype(bf16) for pick in picks]

    def spread(block):
        return jnp.concatenate([block * pick for pick in picks_half], axis=0)

    def fold(block):
        total = block[:seq] * picks[0]
        for e in range(1, per):
            total = total + block[e * seq : (e + 1) * seq] * picks[e]
        return total

    def mix_copy(m, j, c):
        part = mixg.at[m, me, :, mix_cols(c)]
        return remote(part, part, m_s.at[m, j, c], m_r.at[m, me, c], sec, j)

    def on_x(m, j, c):
        part = xin.at[m, j, :, in_cols(c)]
        return remote(part, part, fx_s.at[m, c], x_r.at[m, j, c], sec, peer(n - 1))

    def on_mix(m, j, c):
        part = mixg.at[m, j, :, mix_cols(c)]
        return remote(part, part, fm_s.at[m, c], m_r.at[m, j, c], sec, peer(n - 1))

    def forward(m):
        @pl.when(is_first)
        def _():
            pltpu.make_async_copy(stream.at[m], xin.at[m, me], l_sem.at[m]).wait()

        raw[m] = jnp.zeros(raw.shape[1:], f32)
        sq[...] = jnp.zeros(sq.shape, f32)

        def gathered(step, inside):
            i = visit(step // chunks)
            j = peer(i)
            c = step % chunks

            @pl.when((sec > 0) | (i > 0))
            def _():
                remote(
                    share.at[m, :, in_cols(c)], xin.at[m, j, :, in_cols(c)],
                    x_s.at[m, j, c], x_r.at[m, j, c], sec, j,
                ).wait_recv()

            if relayed:

                @pl.when((i == n - 2) & inner_chip)
                def _():
                    on_x(m, j, c).start()

            piece = xin[m, j, :, in_cols(c)].astype(f32)
            sq[...] += jnp.sum(piece * piece, axis=1, keepdims=True)
            rows = pl.ds(pl.multiple_of(j * width + c * in_half, in_half), in_half)
            scaled = (piece * gain[:, rows]).astype(bf16)
            for at, w in enumerate((wq, wk, wv)):
                raw[m, :, at * inner : (at + 1) * inner] += dot_nn(scaled, w[rows, :])
            return inside

        lax.fori_loop(0, n * chunks, gathered, 0)
        inv = lax.rsqrt(sq[:, :1] / model_width + epsilon)
        inv_kept[m] = jnp.broadcast_to(inv, (seq, 128))
        proj[m] = (raw[m] * inv).astype(bf16)
        mask_row = jnp.where(tokens[pl.ds(m, 1), :] == 0, neg_fill, 0.0)
        for p in range(groups):
            cols = slice(p * 128, (p + 1) * 128)
            q = proj[m, :, p * 128 : (p + 1) * 128]
            k = proj[m, :, inner + p * 128 : inner + (p + 1) * 128]
            v = proj[m, :, 2 * inner + p * 128 : 2 * inner + (p + 1) * 128]
            scores = dot_nt(spread(q), k)
            scores = scores + bias[p * per : (p + 1) * per].reshape(per * seq, seq) + mask_row
            top = jnp.max(scores, axis=-1, keepdims=True)
            grown = jnp.exp(scores - top)
            prob = grown / jnp.sum(grown, axis=-1, keepdims=True)
            probs[m, p] = prob
            mixg[m, me, :, cols] = fold(dot_nn(prob.astype(bf16), v)).astype(bf16)
            if (p + 1) % (groups // chunks) == 0:
                c = p // (groups // chunks)

                @pl.when(sec < sections - 1)
                def _():
                    for i in range(n - 1, 0, -1):
                        unless_far(i, lambda i=i: mix_copy(m, peer(i), c).start())

        @pl.when(is_first & (m + 1 < micro) & (late_x if EARLY else True))
        def _():
            send_x(m + 1)

    def project(m):
        @pl.when(sec < sections - 1)
        def _():
            acc[...] = xin[m, me].astype(f32)

            def mixed(at, inside):
                i = visit(at)
                j = peer(i)

                @pl.when(i > 0)
                def _():
                    for c in range(chunks):
                        part = mixg.at[m, j, :, mix_cols(c)]
                        remote(part, part, m_s.at[m, j, c], m_r.at[m, j, c], sec, j).wait_recv()
                        if relayed:
                            pl.when((i == n - 2) & inner_chip)(on_mix(m, j, c).start)

                rows = pl.ds(pl.multiple_of(j * inner, inner), inner)
                acc[...] += dot_nn(mixg[m, j], wo[rows, :])
                return inside

            lax.fori_loop(0, n, mixed, 0)
            share[m] = acc[...].astype(bf16)
            for c in range(chunks):
                for i in range(n - 1, -1, -1):
                    unless_far(i, lambda i=i, c=c: y_copy(m, peer(i), c).start())

    def i_copy(m, j, c):
        return remote(
            ins.at[m, j, :, in_cols(c)], ip.at[bank, m, me, :, in_cols(c)],
            i_s.at[m, j, c], i_r.at[bank, m, me, c], above, j,
        )

    def r_copy(m, j):
        return remote(
            rads.at[m], rad.at[bank, m, me], r_s.at[m, j], r_r.at[bank, m, me], above, j
        )

    def back_copy(m):
        return remote(gin.at[m], grad.at[m], b_s.at[m], b_r.at[m], sec + 1, me)

    def up_copy(m):
        return remote(gin.at[m], up.at[m], u_s.at[m], u_r.at[m], above, me)

    def t_copy(i):
        other = member(i)
        return pltpu.make_async_remote_copy(
            src_ref=tab.at[mine], dst_ref=tab.at[mine],
            send_sem=t_s.at[other], recv_sem=t_r.at[mine],
            device_id={"section": other // dps, "dp": other % dps}, device_id_type=MESH,
        )

    def d_copy(i):
        other = (dp + i) % dps
        return pltpu.make_async_remote_copy(
            src_ref=gains.at[dp], dst_ref=gains.at[dp],
            send_sem=d_s.at[other], recv_sem=d_r.at[dp],
            device_id={"dp": other}, device_id_type=MESH,
        )

    def e_copy(other):
        return pltpu.make_async_remote_copy(
            src_ref=gains_n, dst_ref=gains.at[dp], send_sem=e_s.at[other], recv_sem=d_r.at[dp],
            device_id={"section": sec + 1, "dp": other}, device_id_type=MESH,
        )

    def combine(m, deep, upstream, rows, gain_part):
        if deep:
            acc[...] = jnp.zeros(acc.shape, f32)
            sq[:8, :seq] = jnp.zeros((8, seq), f32)
        else:
            acc[...] = ins[m, me].astype(f32)
            sq[:8, :seq] = rads[m]

        def arrived_input(i, inside):
            j = peer(i)
            remote(
                rads.at[m], rad.at[deep, m, j], r_s.at[m, j], r_r.at[deep, m, j], sec, j
            ).wait_recv()
            sq[:8, :seq] += rad[deep, m, j]

            def add():
                for c in range(chunks):
                    remote(
                        ins.at[m, j, :, in_cols(c)], ip.at[deep, m, j, :, in_cols(c)],
                        i_s.at[m, j, c], i_r.at[deep, m, j, c], sec, j,
                    ).wait_recv()
                acc[...] += ip[deep, m, j].astype(f32)

            unless_far(i, add)
            return inside

        lax.fori_loop(1 - deep, n, arrived_input, 0)
        inv = rad[1, m, me, 1:2, :] if deep else rads[m, 1:2, :]
        weight = sq[:1, :seq] * inv * inv * inv / model_width
        weight = jnp.broadcast_to(weight, (128, seq)).T[:, :1]
        rows_f32 = rows.astype(f32)
        normed = acc[...]
        result = (upstream.astype(f32) + normed * gain_part - weight * rows_f32).astype(bf16)
        return result, jnp.sum(normed * rows_f32, axis=0, keepdims=True)

    def receive(m):
        @pl.when(m == 0)
        def _():
            pl.when(~flips_first)(flip_all)
            remote(gain_own, gain_n, q_s.at[0], q_r.at[0], sec, me).wait_recv()

        @pl.when(sec < sections - 2)
        def _():
            remote(gin.at[m], up.at[m], u_s.at[m], u_r.at[m], sec, me).wait_recv()

        result, part = combine(m, 1, up[m], share[m], gain_n[...])
        gin[m] = result
        if TOKEN:
            pl.when(dp % 2 == 1)(lambda: pl.semaphore_wait(tok.at[m], 1))
        head_parts(m, gin)
        pass_token(m, 3)
        back_copy(m).start()
        pl.when(sec > 0)(lambda: up_copy(m).start())
        gains_n[...] += part

        @pl.when(m == micro - 1)
        def _():
            for other in range(dps):
                e_copy(other).start()

    def pass_token(m, at):
        if TOKEN == at:

            @pl.when((dp % 2 == 0) & (dp + 1 < dps) & (sec < sections - 1))
            def _():
                pl.semaphore_signal(
                    tok.at[m], inc=1, device_id={"dp": dp + 1}, device_id_type=MESH
                )

    def backward(m):
        mg_ref[...] = hs[m, me].astype(f32)

        def arrived(i, inside):
            j = peer(i)

            def add():
                for c in range(chunks):
                    remote(
                        hs.at[m, j, :, mix_cols(c)], hp.at[m, j, :, mix_cols(c)],
                        h_s.at[m, j, c], h_r.at[m, j, c], sec, j,
                    ).wait_recv()
                mg_ref[...] += hp[m, j].astype(f32)

            unless_far(i, add)
            return inside

        lax.fori_loop(1, n, arrived, 0)
        pass_token(m, 1)
        inv = inv_kept[m][:, :1]
        radial = jnp.zeros((seq, 128), f32)
        for p in range(groups):
            q_cols = slice(p * 128, (p + 1) * 128)
            k_cols = slice(inner + p * 128, inner + (p + 1) * 128)
            v_cols = slice(2 * inner + p * 128, 2 * inner + (p + 1) * 128)
            q2 = spread(proj[m, :, q_cols])
            k = proj[m, :, k_cols]
            v = proj[m, :, v_cols]
            mg2 = spread(mg_ref[:, q_cols].astype(bf16))
            prob = probs[m, p]
            prob_grad = dot_nt(mg2, v)
            value_grad = dot_tn(prob.astype(bf16), mg2)
            score_grad = prob * (prob_grad - jnp.sum(prob_grad * prob, axis=-1, keepdims=True))
            wide = jnp.concatenate([score_grad, jnp.zeros_like(score_grad)], axis=1)
            for e in range(per):
                part = wide[e * seq : e * seq + 8]
                for a in range(8, seq, 8):
                    part = part + pltpu.roll(
                        wide[e * seq + a : e * seq + a + 8], (2 * seq - a) % (2 * seq), 1
                    )
                diag[p * per + e] += part
            half = score_grad.astype(bf16)
            query_grad = fold(dot_nn(half, k))
            key_grad = dot_tn(half, q2)
            for cols, part in ((q_cols, query_grad), (k_cols, key_grad), (v_cols, value_grad)):
                radial = radial + part * raw[m, :, cols]
                sgr[:, cols] = (part * inv).astype(bf16)
        rads[m] = jnp.where(lane == 0, jnp.sum(radial, axis=1, keepdims=True), inv).T[:8]
        for i in range(n - 1, 0, -1):
            r_copy(m, peer(i)).start()
        pl.when(sec > 0)(lambda: r_copy(m, me).start())

        def input_part(step, inside):
            i = emit(step // chunks)
            c = step % chunks
            at = pl.ds(pl.multiple_of(peer(i) * width + c * in_half, in_half), in_half)
            part = dot_nn(sgr[:, :inner], wq_t[:, at])
            part += dot_nn(sgr[:, inner : 2 * inner], wk_t[:, at])
            part += dot_nn(sgr[:, 2 * inner :], wv_t[:, at])
            pass_on(m, i, c, in_cols(c), part, ins, ex_i, i_s, ei_r, i_copy, sec > 0)
            return inside

        lax.fori_loop(0, n * chunks, input_part, 0)
        pass_token(m, 2)

        @pl.when(m == micro - 1)
        def _():
            sub = lax.broadcasted_iota(jnp.int32, (8, 2 * seq), 0)
            for h in range(heads):
                part = diag[h]
                for bit in (1, 2, 4):
                    moved = pltpu.roll(part, 2 * seq - bit, 1)
                    part = jnp.where((sub // bit) % 2 == 1, moved, part)
                tab[mine, h : h + 1] = jnp.sum(part, axis=0, keepdims=True)
            for i in range(1, everyone):
                t_copy(i).start()

    def finish_table():
        def table_wait(i, carry):
            other = member(i)
            pltpu.make_async_remote_copy(
                src_ref=tab.at[mine], dst_ref=tab.at[other],
                send_sem=t_s.at[other], recv_sem=t_r.at[other],
                device_id={"section": other // dps, "dp": other % dps}, device_id_type=MESH,
            ).wait()
            return carry

        lax.fori_loop(1, everyone, table_wait, 0)
        total = tab[0]
        for at in range(1, everyone):
            total = total + tab[at]
        last = buckets[seq - 1 : seq, :]
        place = jnp.concatenate([buckets[0:1, :], last[:, seq - 1 :], last[:, : seq - 1]], axis=1)
        summed = jnp.zeros(total.shape, f32)
        for c in range(table.shape[1]):
            part = jnp.sum(jnp.where(place == c, total, 0.0), axis=1, keepdims=True)
            summed = jnp.where(lane == c, part, summed)
        table_out[...] = summed[:heads, : table_out.shape[1]]
    def settle(m):
        pl.when(m == micro - 1)(finish_table)
        result, part = combine(m, 0, gin[m], xin[m, me], gain_own[...])
        grads_out[0, m] = result
        gains[dp] += part

    def step(t, carry):
        u = t - 2 * micro
        v = t - 4 * micro
        kind = jnp.where(u < 0, t % 2, jnp.where(v < 0, u % 2 + 2, 4))
        m = jnp.where(u < 0, t // 2, jnp.where(v < 0, u // 2, v))
        kind = jnp.where(is_last, t % 2 * 3, kind)
        m = jnp.where(is_last, t // 2, m)
        busy = (t < 4 * micro) & (~is_last | (t < 2 * micro)) | is_first

        for at, act in enumerate((forward, project, receive, backward, settle)):
            pl.when((kind == at) & busy)(lambda act=act: act(m))

        return carry

    lax.fori_loop(0, 5 * micro, step, 0)

    @pl.when(is_first)
    def _():
        for i in range(1, dps):
            d_copy(i).start()

    @pl.when(sec > 0)
    def _():
        q_copy().wait_send()
        for m in range(micro):
            remote(gin.at[m], grad.at[m], b_s.at[m], b_r.at[m], sec, me).wait_recv()
            grads_out[0, m] = grad[m]
            r_copy(m, me).wait_send()
            for c in range(chunks):
                i_copy(m, me, c).wait_send()

    @pl.when(sec < sections - 1)
    def _():
        for m in range(micro):
            back_copy(m).wait_send()
            pl.when(sec > 0)(up_copy(m).wait_send)
        for other in range(dps):
            e_copy(other).wait_send()

    def finish(m, carry):
        def one(i, inside):
            j = peer(i)
            r_copy(m, j).wait_send()
            for c in range(chunks):
                h_copy(m, j, c).wait_send()
                i_copy(m, j, c).wait_send()

                @pl.when(is_first)
                def _():
                    unless_far(i, x_copy(m, j, c).wait_send)

                @pl.when(sec < sections - 1)
                def _():
                    unless_far(i, mix_copy(m, j, c).wait_send)

            return inside

        lax.fori_loop(1, n, one, 0)
        if relayed:

            for c in range(chunks):
                pl.when(inner_chip)(on_x(m, peer(n - 2), c).wait_send)
                pl.when(inner_chip & (sec < sections - 1))(on_mix(m, peer(n - 2), c).wait_send)

        return carry

    lax.fori_loop(0, micro, finish, 0)

    @pl.when(sec < sections - 1)
    def _():
        def one(m, carry):
            for i in range(n):
                for c in range(chunks):
                    unless_far(i, y_copy(m, peer(i), c).wait_send)
            return carry

        lax.fori_loop(0, micro, one, 0)

    pl.when(sec > 0)(finish_table)

    def gain_in(other):
        return pltpu.make_async_remote_copy(
            src_ref=gains.at[dp], dst_ref=gains.at[other],
            send_sem=d_s.at[other], recv_sem=d_r.at[other],
            device_id={"dp": other}, device_id_type=MESH,
        )

    for i in range(1, dps):
        other = (dp + i) % dps
        gain_in(other).wait_recv()
        pl.when(is_first)(gain_in(other).wait_send)
    pl.when(sec > 0)(gain_in(dp).wait_recv)
    total = gains[0]
    for at in range(1, dps):
        total = total + gains[at]
    gain_out[...] = total


def hand_on(grads, gains, table, grads_out, gains_out, table_out):
    grads_out[...] = grads[...]
    gains_out[...] = gains[...]
    table_out[...] = table[...]


def per_device(
    stream, cotangent, token_ids, buckets, bias_table, gain, w_query, w_key, w_value, w_out
):
    sections = lax.axis_size("section")
    n = lax.axis_size("mp")
    dps = lax.axis_size("dp")
    micro, seq, width = stream.shape
    heads = bias_table.shape[1]
    inner = w_query.shape[2]
    head_dim = inner // heads
    groups = heads * head_dim // 128
    per = 128 // head_dim
    vmem = pl.BlockSpec(memory_space=pltpu.VMEM)
    hbm = pl.BlockSpec(memory_space=pl.ANY)
    dma = pltpu.SemaphoreType.DMA
    grads, gains, table_grad = pl.pallas_call(
        functools.partial(relay_kernel, sections, n, dps, head_dim),
        out_shape=(
            jax.ShapeDtypeStruct((1, micro, seq, width), bf16),
            jax.ShapeDtypeStruct((1, width), f32),
            jax.ShapeDtypeStruct(bias_table.shape[::-1], f32),
        ),
        in_specs=[vmem, vmem, vmem, vmem, pl.BlockSpec(memory_space=pltpu.SMEM), vmem]
        + [hbm] * 4,
        out_specs=(vmem, vmem, vmem),
        scratch_shapes=[
            pltpu.VMEM(w_query.shape[1:], bf16),
            pltpu.VMEM(w_key.shape[1:], bf16),
            pltpu.VMEM(w_value.shape[1:], bf16),
            pltpu.VMEM(w_out.shape[1:], bf16),
            pltpu.VMEM(w_query.shape[:0:-1], bf16),
            pltpu.VMEM(w_key.shape[:0:-1], bf16),
            pltpu.VMEM(w_value.shape[:0:-1], bf16),
            pltpu.VMEM(w_out.shape[:0:-1], bf16),
            pltpu.VMEM((heads, seq, seq), f32),
            pltpu.VMEM((micro, n, seq, width), bf16),
            pltpu.VMEM((micro, n, seq, inner), bf16),
            pltpu.VMEM((micro, n, seq, inner), bf16),
            pltpu.VMEM((2, micro, n, seq, width), bf16),
            pltpu.VMEM((2, micro, n, 8, seq), f32),
            pltpu.VMEM((micro, seq, width), bf16),
            pltpu.VMEM((micro, n, seq, inner), bf16),
            pltpu.VMEM((micro, n, seq, width), bf16),
            pltpu.VMEM((micro, 8, seq), f32),
            pltpu.VMEM((micro, seq, width), bf16),
            pltpu.VMEM((micro, seq, width), bf16),
            pltpu.VMEM((micro, seq, width), bf16),
            pltpu.VMEM((1, width), f32),
            pltpu.VMEM((1, width), f32),
            pltpu.VMEM((1, width), f32),
            pltpu.VMEM((micro, seq, 3 * inner), f32),
            pltpu.VMEM((micro, seq, 3 * inner), bf16),
            pltpu.VMEM((micro, groups, per * seq, seq), f32),
            pltpu.VMEM((micro, seq, 128), f32),
            pltpu.VMEM((seq, width), f32),
            pltpu.VMEM((seq, inner), f32),
            pltpu.VMEM((seq, 3 * inner), bf16),
            pltpu.VMEM((seq, 128), f32),
            pltpu.VMEM((heads, 8, 2 * seq), f32),
            pltpu.VMEM((sections * dps, max(heads, 8), 2 * seq), f32),
            pltpu.VMEM((dps, 1, width), f32),
            pltpu.VMEM((micro, seq, inner), bf16),
            pltpu.VMEM((micro, seq, width), bf16),
            dma((4,)),
            dma((micro,)),
        ]
        + [dma((micro, n, CHUNKS))] * 8
        + [dma((2, micro, n, CHUNKS)), dma((micro, n)), dma((2, micro, n))]
        + [dma((micro,))] * 4
        + [dma((1,))] * 2
        + [dma((dps,))]
        + [dma((sections * dps,))] * 2
        + [dma((dps,))] * 2
        + [dma((micro, CHUNKS))] * 4
        + [pltpu.SemaphoreType.REGULAR((micro,))],
        compiler_params=pltpu.CompilerParams(
            collective_id=0, has_side_effects=True, vmem_limit_bytes=60 * 1024 * 1024
        ),
    )(
        stream, cotangent, token_ids, buckets, bias_table.T, gain, w_query, w_key, w_value, w_out,
    )
    grads, gains, table_grad = pl.pallas_call(
        hand_on,
        out_shape=(
            jax.ShapeDtypeStruct(grads.shape, bf16),
            jax.ShapeDtypeStruct(gains.shape, f32),
            jax.ShapeDtypeStruct(table_grad.shape, f32),
        ),
        in_specs=[vmem] * 3,
        out_specs=(vmem,) * 3,
    )(grads, gains, table_grad)
    return grads, gains, table_grad.T


def solution(mesh):
    in_specs = (
        P("dp", None, "mp"),
        P("dp", None, "mp"),
        P("dp", None),
        P(),
        P(None, "mp"),
        P("section", None),
        P("section", None, "mp"),
        P("section", None, "mp"),
        P("section", None, "mp"),
        P("section", None, "mp"),
    )
    out_specs = (P("section", "dp", None, "mp"), P("section", "mp"), P(None, "mp"))
    return jax.shard_map(
        per_device, mesh=mesh, in_specs=in_specs, out_specs=out_specs, check_vma=False
    )
```

```python
import functools

import jax
import jax.numpy as jnp
from jax import lax
from jax.experimental import pallas as pl
from jax.experimental.pallas import tpu as pltpu
from jax.sharding import PartitionSpec as P

neg_fill = -1000000000.0
epsilon = 1e-06
MESH = pl.DeviceIdType.MESH
DELAY = 12000
DELAYED = 1
EARLY = True
CHUNKS = 4
TOKEN = 0
f32 = jnp.float32
bf16 = jnp.bfloat16


def dot_nn(a, b):
    return lax.dot_general(a, b, (((1,), (0,)), ((), ())), preferred_element_type=f32)


def dot_nt(a, b):
    return lax.dot_general(a, b, (((1,), (1,)), ((), ())), preferred_element_type=f32)


def dot_tn(a, b):
    return lax.dot_general(a, b, (((0,), (0,)), ((), ())), preferred_element_type=f32)


def relay_kernel(
    sections, n, dps, head_dim,
    stream, cotangent, tokens, buckets, table, gain, wq_hbm, wk_hbm, wv_hbm, wo_hbm,
    grads_out, gain_out, table_out,
    wq, wk, wv, wo, wq_t, wk_t, wv_t, wo_t, bias, xin, mixg, hp, ip, rad, gin, hs, ins, rads, share, grad, up, gain_own, gain_n, gains_n,
    raw, proj, probs, inv_kept, acc, mg_ref, sgr, sq, diag, tab, gains, ex_h, ex_i,
    w_sem, l_sem, x_s, y_s, x_r, m_s, m_r, h_s, h_r, i_s, i_r, r_s, r_r, b_s, b_r, u_s, u_r, q_s, q_r, e_s, t_s, t_r, d_s, d_r, fx_s, fm_s, eh_r, ei_r, tok,
):
    micro, seq, width = stream.shape
    heads = bias.shape[0]
    inner = heads * head_dim
    per = 128 // head_dim
    groups = heads // per
    model_width = n * width
    sec = lax.axis_index("section")
    me = lax.axis_index("mp")
    dp = lax.axis_index("dp")
    everyone = sections * dps
    mine = sec * dps + dp
    turn = 1 - 2 * (me // ((n + 1) // 2))

    def peer(i):
        return (me + i * turn + n) % n

    relayed = n == 4
    chunks = CHUNKS if relayed and inner % 512 == 0 and width % 512 == 0 else 1
    in_half, mix_half = width // chunks, inner // chunks

    def in_cols(c):
        return pl.ds(pl.multiple_of(c * in_half, in_half), in_half)

    def mix_cols(c):
        return pl.ds(pl.multiple_of(c * mix_half, mix_half), mix_half)

    def flip(src, dst):
        rows = min(256, src.shape[0])

        def one(r, carry):
            at = pl.ds(pl.multiple_of(r * rows, rows), rows)
            dst[:, at] = src[at, :].T
            return carry

        lax.fori_loop(0, src.shape[0] // rows, one, 0)

    def flip_all():
        for src, dst in ((wo, wo_t), (wq, wq_t), (wk, wk_t), (wv, wv_t)):
            flip(src, dst)

    flips_first = sec * 2 >= sections
    inner_chip = (me % (n - 1)) != 0 if relayed else True

    def visit(at):
        return jnp.where(at == 1, 2, jnp.where(at == 2, 1, at)) if relayed else at

    def unless_far(i, act):
        if relayed:
            pl.when((i < n - 1) | inner_chip)(act)
        else:
            act()

    def remote(src, dst, ssem, rsem, to_sec, to_mp):
        return pltpu.make_async_remote_copy(
            src_ref=src, dst_ref=dst, send_sem=ssem, recv_sem=rsem,
            device_id={"section": to_sec, "mp": to_mp}, device_id_type=MESH,
        )

    loads = [
        pltpu.make_async_copy(src, dst, w_sem.at[at])
        for at, (src, dst) in enumerate(
            ((wq_hbm.at[0], wq), (wk_hbm.at[0], wk), (wv_hbm.at[0], wv), (wo_hbm.at[0], wo))
        )
    ]
    for load in loads:
        load.start()

    barrier = pltpu.get_barrier_semaphore()
    is_first = sec == 0
    is_last = sec == sections - 1
    for i in range(1, n):
        pl.semaphore_signal(
            barrier, inc=1, device_id={"section": sec, "mp": peer(i)}, device_id_type=MESH
        )

    @pl.when(sec > 0)
    def _():
        for j in range(n):
            pl.semaphore_signal(
                barrier, inc=1, device_id={"section": sec - 1, "mp": j}, device_id_type=MESH
            )

    @pl.when(sec < sections - 1)
    def _():
        for j in range(n):
            pl.semaphore_signal(
                barrier, inc=1, device_id={"section": sec + 1, "mp": j}, device_id_type=MESH
            )

    def member(i):
        return (mine + i) % everyone

    for i in range(1, everyone):
        other = member(i)
        pl.semaphore_signal(
            barrier, inc=1, device_id={"section": other // dps, "dp": other % dps},
            device_id_type=MESH,
        )

    greeters = n - 1 + everyone - 1 + n * jnp.minimum(sec, 1) + n * jnp.minimum(sections - 1 - sec, 1)
    pl.semaphore_wait(barrier, greeters)

    above = jnp.maximum(sec - 1, 0)
    bank = jnp.minimum(sec, 1)

    def q_copy():
        return remote(gain_own, gain_n, q_s.at[0], q_r.at[0], above, me)

    gain_own[...] = gain[:, pl.ds(pl.multiple_of(me * width, width), width)]
    pl.when(sec > 0)(lambda: q_copy().start())
    gains_n[...] = jnp.zeros(gains_n.shape, f32)

    @pl.when(sec == sections - 2)
    def _():
        up[...] = cotangent[...]

    def x_copy(m, j, c):
        return remote(
            stream.at[m, :, in_cols(c)], xin.at[m, me, :, in_cols(c)],
            x_s.at[m, j, c], x_r.at[m, me, c], sec, j,
        )

    def y_copy(m, j, c):
        return remote(
            share.at[m, :, in_cols(c)], xin.at[m, me, :, in_cols(c)],
            y_s.at[m, j, c], x_r.at[m, me, c], sec + 1, j,
        )

    late_x = dp % 2 == 1

    def send_x(m):
        pltpu.make_async_copy(stream.at[m], xin.at[m, me], l_sem.at[m]).start()
        for c in range(chunks):
            for i in range(n - 1, 0, -1):
                unless_far(i, lambda i=i, c=c: x_copy(m, peer(i), c).start())

    @pl.when(is_first)
    def _():
        @pl.when(dp % 2 == DELAYED)
        def _():
            pl.delay(DELAY)

        send_x(0)
        if EARLY:
            for m in range(1, micro):
                pl.when(dp % 2 == 0)(functools.partial(send_x, m))

    def head_bias(h, carry):
        value = jnp.zeros((seq, seq), f32)
        held = buckets[...]
        for c in range(table.shape[1]):
            value = jnp.where(held == c, table[h, c], value)
        bias[h] = value
        return carry

    lax.fori_loop(0, heads, head_bias, 0)
    tab[mine] = jnp.zeros(tab.shape[1:], f32)
    diag[...] = jnp.zeros(diag.shape, f32)
    gains[dp] = jnp.zeros(gains.shape[1:], f32)
    for load in loads:
        load.wait()
    pl.when(flips_first)(flip_all)

    def h_copy(m, j, c):
        return remote(
            hs.at[m, j, :, mix_cols(c)], hp.at[m, me, :, mix_cols(c)],
            h_s.at[m, j, c], h_r.at[m, me, c], sec, j,
        )

    def emit(at):
        return jnp.where(at == 0, 3, jnp.where(at == 3, 2, 2 - at)) if relayed else n - 1 - at

    def pass_on(m, i, c, cols, part, own, extra, own_sem, extra_sem, copy, lifted):
        j = peer(i)
        own[m, j, :, cols] = part.astype(bf16)
        if not relayed:
            pl.when((i > 0) | lifted)(lambda: copy(m, j, c).start())
            return

        def hand_over():
            return remote(
                own.at[m, j, :, cols], extra.at[m, :, cols],
                own_sem.at[m, j, c], extra_sem.at[m, c], sec, peer(1),
            )

        @pl.when((i == n - 2) & inner_chip)
        def _():
            hand_over().wait_recv()
            own[m, j, :, cols] = (part + extra[m, :, cols].astype(f32)).astype(bf16)

        @pl.when(((i > 0) | lifted) & ((i < n - 1) | inner_chip))
        def _():
            copy(m, j, c).start()

        @pl.when((i == n - 1) & ((me % (n - 1)) == 0))
        def _():
            hand_over().start()

    def head_parts(m, upstream):
        def one(step, carry):
            i = emit(step)
            j = peer(i)
            cols = pl.ds(pl.multiple_of(j * inner, inner), inner)
            part = dot_nn(upstream[m], wo_t[:, cols])
            for c in range(chunks):
                at = slice(c * mix_half, (c + 1) * mix_half)
                pass_on(m, i, c, at, part[:, at], hs, ex_h, h_s, eh_r, h_copy, False)
            return carry

        lax.fori_loop(0, n, one, 0)

    @pl.when(is_last)
    def _():
        def one(m, carry):
            head_parts(m, cotangent)
            return carry

        lax.fori_loop(0, micro, one, 0)

    lane = lax.broadcasted_iota(jnp.int32, (1, 128), 1)
    picks = [
        jnp.where((lane // head_dim) == e, 1.0, 0.0).astype(f32) for e in range(per)
    ]
    picks_half = [pick.astype(bf16) for pick in picks]

    def spread(block):
        return jnp.concatenate([block * pick for pick in picks_half], axis=0)

    def fold(block):
        total = block[:seq] * picks[0]
        for e in range(1, per):
            total = total + block[e * seq : (e + 1) * seq] * picks[e]
        return total

    def mix_copy(m, j, c):
        part = mixg.at[m, me, :, mix_cols(c)]
        return remote(part, part, m_s.at[m, j, c], m_r.at[m, me, c], sec, j)

    def on_x(m, j, c):
        part = xin.at[m, j, :, in_cols(c)]
        return remote(part, part, fx_s.at[m, c], x_r.at[m, j, c], sec, peer(n - 1))

    def on_mix(m, j, c):
        part = mixg.at[m, j, :, mix_cols(c)]
        return remote(part, part, fm_s.at[m, c], m_r.at[m, j, c], sec, peer(n - 1))

    def forward(m):
        @pl.when(is_first)
        def _():
            pltpu.make_async_copy(stream.at[m], xin.at[m, me], l_sem.at[m]).wait()

        raw[m] = jnp.zeros(raw.shape[1:], f32)
        sq[...] = jnp.zeros(sq.shape, f32)

        def gathered(step, inside):
            i = visit(step // chunks)
            j = peer(i)
            c = step % chunks

            @pl.when((sec > 0) | (i > 0))
            def _():
                remote(
                    share.at[m, :, in_cols(c)], xin.at[m, j, :, in_cols(c)],
                    x_s.at[m, j, c], x_r.at[m, j, c], sec, j,
                ).wait_recv()

            if relayed:

                @pl.when((i == n - 2) & inner_chip)
                def _():
                    on_x(m, j, c).start()

            piece = xin[m, j, :, in_cols(c)].astype(f32)
            sq[...] += jnp.sum(piece * piece, axis=1, keepdims=True)
            rows = pl.ds(pl.multiple_of(j * width + c * in_half, in_half), in_half)
            scaled = (piece * gain[:, rows]).astype(bf16)
            for at, w in enumerate((wq, wk, wv)):
                raw[m, :, at * inner : (at + 1) * inner] += dot_nn(scaled, w[rows, :])
            return inside

        lax.fori_loop(0, n * chunks, gathered, 0)
        inv = lax.rsqrt(sq[:, :1] / model_width + epsilon)
        inv_kept[m] = jnp.broadcast_to(inv, (seq, 128))
        proj[m] = (raw[m] * inv).astype(bf16)
        mask_row = jnp.where(tokens[pl.ds(m, 1), :] == 0, neg_fill, 0.0)
        for p in range(groups):
            cols = slice(p * 128, (p + 1) * 128)
            q = proj[m, :, p * 128 : (p + 1) * 128]
            k = proj[m, :, inner + p * 128 : inner + (p + 1) * 128]
            v = proj[m, :, 2 * inner + p * 128 : 2 * inner + (p + 1) * 128]
            scores = dot_nt(spread(q), k)
            scores = scores + bias[p * per : (p + 1) * per].reshape(per * seq, seq) + mask_row
            top = jnp.max(scores, axis=-1, keepdims=True)
            grown = jnp.exp(scores - top)
            prob = grown / jnp.sum(grown, axis=-1, keepdims=True)
            probs[m, p] = prob
            mixg[m, me, :, cols] = fold(dot_nn(prob.astype(bf16), v)).astype(bf16)
            if (p + 1) % (groups // chunks) == 0:
                c = p // (groups // chunks)

                @pl.when(sec < sections - 1)
                def _():
                    for i in range(n - 1, 0, -1):
                        unless_far(i, lambda i=i: mix_copy(m, peer(i), c).start())

        @pl.when(is_first & (m + 1 < micro) & (late_x if EARLY else True))
        def _():
            send_x(m + 1)

    def project(m):
        @pl.when(sec < sections - 1)
        def _():
            acc[...] = xin[m, me].astype(f32)

            def mixed(at, inside):
                i = visit(at)
                j = peer(i)

                @pl.when(i > 0)
                def _():
                    for c in range(chunks):
                        part = mixg.at[m, j, :, mix_cols(c)]
                        remote(part, part, m_s.at[m, j, c], m_r.at[m, j, c], sec, j).wait_recv()
                        if relayed:
                            pl.when((i == n - 2) & inner_chip)(on_mix(m, j, c).start)

                rows = pl.ds(pl.multiple_of(j * inner, inner), inner)
                acc[...] += dot_nn(mixg[m, j], wo[rows, :])
                return inside

            lax.fori_loop(0, n, mixed, 0)
            share[m] = acc[...].astype(bf16)
            for c in range(chunks):
                for i in range(n - 1, -1, -1):
                    unless_far(i, lambda i=i, c=c: y_copy(m, peer(i), c).start())

    def i_copy(m, j, c):
        return remote(
            ins.at[m, j, :, in_cols(c)], ip.at[bank, m, me, :, in_cols(c)],
            i_s.at[m, j, c], i_r.at[bank, m, me, c], above, j,
        )

    def r_copy(m, j):
        return remote(
            rads.at[m], rad.at[bank, m, me], r_s.at[m, j], r_r.at[bank, m, me], above, j
        )

    def back_copy(m):
        return remote(gin.at[m], grad.at[m], b_s.at[m], b_r.at[m], sec + 1, me)

    def up_copy(m):
        return remote(gin.at[m], up.at[m], u_s.at[m], u_r.at[m], above, me)

    def t_copy(i):
        other = member(i)
        return pltpu.make_async_remote_copy(
            src_ref=tab.at[mine], dst_ref=tab.at[mine],
            send_sem=t_s.at[other], recv_sem=t_r.at[mine],
            device_id={"section": other // dps, "dp": other % dps}, device_id_type=MESH,
        )

    def d_copy(i):
        other = (dp + i) % dps
        return pltpu.make_async_remote_copy(
            src_ref=gains.at[dp], dst_ref=gains.at[dp],
            send_sem=d_s.at[other], recv_sem=d_r.at[dp],
            device_id={"dp": other}, device_id_type=MESH,
        )

    def e_copy(other):
        return pltpu.make_async_remote_copy(
            src_ref=gains_n, dst_ref=gains.at[dp], send_sem=e_s.at[other], recv_sem=d_r.at[dp],
            device_id={"section": sec + 1, "dp": other}, device_id_type=MESH,
        )

    def combine(m, deep, upstream, rows, gain_part):
        if deep:
            acc[...] = jnp.zeros(acc.shape, f32)
            sq[:8, :seq] = jnp.zeros((8, seq), f32)
        else:
            acc[...] = ins[m, me].astype(f32)
            sq[:8, :seq] = rads[m]

        def arrived_input(i, inside):
            j = peer(i)
            remote(
                rads.at[m], rad.at[deep, m, j], r_s.at[m, j], r_r.at[deep, m, j], sec, j
            ).wait_recv()
            sq[:8, :seq] += rad[deep, m, j]

            def add():
                for c in range(chunks):
                    remote(
                        ins.at[m, j, :, in_cols(c)], ip.at[deep, m, j, :, in_cols(c)],
                        i_s.at[m, j, c], i_r.at[deep, m, j, c], sec, j,
                    ).wait_recv()
                acc[...] += ip[deep, m, j].astype(f32)

            unless_far(i, add)
            return inside

        lax.fori_loop(1 - deep, n, arrived_input, 0)
        inv = rad[1, m, me, 1:2, :] if deep else rads[m, 1:2, :]
        weight = sq[:1, :seq] * inv * inv * inv / model_width
        weight = jnp.broadcast_to(weight, (128, seq)).T[:, :1]
        rows_f32 = rows.astype(f32)
        normed = acc[...]
        result = (upstream.astype(f32) + normed * gain_part - weight * rows_f32).astype(bf16)
        return result, jnp.sum(normed * rows_f32, axis=0, keepdims=True)

    def receive(m):
        @pl.when(m == 0)
        def _():
            pl.when(~flips_first)(flip_all)
            remote(gain_own, gain_n, q_s.at[0], q_r.at[0], sec, me).wait_recv()

        @pl.when(sec < sections - 2)
        def _():
            remote(gin.at[m], up.at[m], u_s.at[m], u_r.at[m], sec, me).wait_recv()

        result, part = combine(m, 1, up[m], share[m], gain_n[...])
        gin[m] = result
        if TOKEN:
            pl.when(dp % 2 == 1)(lambda: pl.semaphore_wait(tok.at[m], 1))
        head_parts(m, gin)
        pass_token(m, 3)
        pl.when(sec > 0)(lambda: up_copy(m).start())
        gains_n[...] += part

        @pl.when(m == micro - 1)
        def _():
            for other in range(dps):
                e_copy(other).start()

    def pass_token(m, at):
        if TOKEN == at:

            @pl.when((dp % 2 == 0) & (dp + 1 < dps) & (sec < sections - 1))
            def _():
                pl.semaphore_signal(
                    tok.at[m], inc=1, device_id={"dp": dp + 1}, device_id_type=MESH
                )

    def backward(m):
        mg_ref[...] = hs[m, me].astype(f32)

        def arrived(i, inside):
            j = peer(i)

            def add():
                for c in range(chunks):
                    remote(
                        hs.at[m, j, :, mix_cols(c)], hp.at[m, j, :, mix_cols(c)],
                        h_s.at[m, j, c], h_r.at[m, j, c], sec, j,
                    ).wait_recv()
                mg_ref[...] += hp[m, j].astype(f32)

            unless_far(i, add)
            return inside

        lax.fori_loop(1, n, arrived, 0)
        pass_token(m, 1)
        inv = inv_kept[m][:, :1]
        radial = jnp.zeros((seq, 128), f32)
        for p in range(groups):
            q_cols = slice(p * 128, (p + 1) * 128)
            k_cols = slice(inner + p * 128, inner + (p + 1) * 128)
            v_cols = slice(2 * inner + p * 128, 2 * inner + (p + 1) * 128)
            q2 = spread(proj[m, :, q_cols])
            k = proj[m, :, k_cols]
            v = proj[m, :, v_cols]
            mg2 = spread(mg_ref[:, q_cols].astype(bf16))
            prob = probs[m, p]
            prob_grad = dot_nt(mg2, v)
            value_grad = dot_tn(prob.astype(bf16), mg2)
            score_grad = prob * (prob_grad - jnp.sum(prob_grad * prob, axis=-1, keepdims=True))
            wide = jnp.concatenate([score_grad, jnp.zeros_like(score_grad)], axis=1)
            for e in range(per):
                part = wide[e * seq : e * seq + 8]
                for a in range(8, seq, 8):
                    part = part + pltpu.roll(
                        wide[e * seq + a : e * seq + a + 8], (2 * seq - a) % (2 * seq), 1
                    )
                diag[p * per + e] += part
            half = score_grad.astype(bf16)
            query_grad = fold(dot_nn(half, k))
            key_grad = dot_tn(half, q2)
            for cols, part in ((q_cols, query_grad), (k_cols, key_grad), (v_cols, value_grad)):
                radial = radial + part * raw[m, :, cols]
                sgr[:, cols] = (part * inv).astype(bf16)
        rads[m] = jnp.where(lane == 0, jnp.sum(radial, axis=1, keepdims=True), inv).T[:8]
        for i in range(n - 1, 0, -1):
            r_copy(m, peer(i)).start()
        pl.when(sec > 0)(lambda: r_copy(m, me).start())

        def input_part(step, inside):
            i = emit(step // chunks)
            c = step % chunks
            at = pl.ds(pl.multiple_of(peer(i) * width + c * in_half, in_half), in_half)
            part = dot_nn(sgr[:, :inner], wq_t[:, at])
            part += dot_nn(sgr[:, inner : 2 * inner], wk_t[:, at])
            part += dot_nn(sgr[:, 2 * inner :], wv_t[:, at])
            pass_on(m, i, c, in_cols(c), part, ins, ex_i, i_s, ei_r, i_copy, sec > 0)
            return inside

        lax.fori_loop(0, n * chunks, input_part, 0)
        pl.when(sec < sections - 1)(lambda: back_copy(m).start())
        pass_token(m, 2)

        @pl.when(m == micro - 1)
        def _():
            sub = lax.broadcasted_iota(jnp.int32, (8, 2 * seq), 0)
            for h in range(heads):
                part = diag[h]
                for bit in (1, 2, 4):
                    moved = pltpu.roll(part, 2 * seq - bit, 1)
                    part = jnp.where((sub // bit) % 2 == 1, moved, part)
                tab[mine, h : h + 1] = jnp.sum(part, axis=0, keepdims=True)
            for i in range(1, everyone):
                t_copy(i).start()

    def finish_table():
        def table_wait(i, carry):
            other = member(i)
            pltpu.make_async_remote_copy(
                src_ref=tab.at[mine], dst_ref=tab.at[other],
                send_sem=t_s.at[other], recv_sem=t_r.at[other],
                device_id={"section": other // dps, "dp": other % dps}, device_id_type=MESH,
            ).wait()
            return carry

        lax.fori_loop(1, everyone, table_wait, 0)
        total = tab[0]
        for at in range(1, everyone):
            total = total + tab[at]
        last = buckets[seq - 1 : seq, :]
        place = jnp.concatenate([buckets[0:1, :], last[:, seq - 1 :], last[:, : seq - 1]], axis=1)
        summed = jnp.zeros(total.shape, f32)
        for c in range(table.shape[1]):
            part = jnp.sum(jnp.where(place == c, total, 0.0), axis=1, keepdims=True)
            summed = jnp.where(lane == c, part, summed)
        table_out[...] = summed[:heads, : table_out.shape[1]]
    def settle(m):
        pl.when(m == micro - 1)(finish_table)
        result, part = combine(m, 0, gin[m], xin[m, me], gain_own[...])
        grads_out[0, m] = result
        gains[dp] += part

    def step(t, carry):
        u = t - 2 * micro
        v = t - 4 * micro
        kind = jnp.where(u < 0, t % 2, jnp.where(v < 0, u % 2 + 2, 4))
        m = jnp.where(u < 0, t // 2, jnp.where(v < 0, u // 2, v))
        kind = jnp.where(is_last, t % 2 * 3, kind)
        m = jnp.where(is_last, t // 2, m)
        busy = (t < 4 * micro) & (~is_last | (t < 2 * micro)) | is_first

        for at, act in enumerate((forward, project, receive, backward, settle)):
            pl.when((kind == at) & busy)(lambda act=act: act(m))

        return carry

    lax.fori_loop(0, 5 * micro, step, 0)

    @pl.when(is_first)
    def _():
        for i in range(1, dps):
            d_copy(i).start()

    @pl.when(sec > 0)
    def _():
        q_copy().wait_send()
        for m in range(micro):
            remote(gin.at[m], grad.at[m], b_s.at[m], b_r.at[m], sec, me).wait_recv()
            grads_out[0, m] = grad[m]
            r_copy(m, me).wait_send()
            for c in range(chunks):
                i_copy(m, me, c).wait_send()

    @pl.when(sec < sections - 1)
    def _():
        for m in range(micro):
            back_copy(m).wait_send()
            pl.when(sec > 0)(up_copy(m).wait_send)
        for other in range(dps):
            e_copy(other).wait_send()

    def finish(m, carry):
        def one(i, inside):
            j = peer(i)
            r_copy(m, j).wait_send()
            for c in range(chunks):
                h_copy(m, j, c).wait_send()
                i_copy(m, j, c).wait_send()

                @pl.when(is_first)
                def _():
                    unless_far(i, x_copy(m, j, c).wait_send)

                @pl.when(sec < sections - 1)
                def _():
                    unless_far(i, mix_copy(m, j, c).wait_send)

            return inside

        lax.fori_loop(1, n, one, 0)
        if relayed:

            for c in range(chunks):
                pl.when(inner_chip)(on_x(m, peer(n - 2), c).wait_send)
                pl.when(inner_chip & (sec < sections - 1))(on_mix(m, peer(n - 2), c).wait_send)

        return carry

    lax.fori_loop(0, micro, finish, 0)

    @pl.when(sec < sections - 1)
    def _():
        def one(m, carry):
            for i in range(n):
                for c in range(chunks):
                    unless_far(i, y_copy(m, peer(i), c).wait_send)
            return carry

        lax.fori_loop(0, micro, one, 0)

    pl.when(sec > 0)(finish_table)

    def gain_in(other):
        return pltpu.make_async_remote_copy(
            src_ref=gains.at[dp], dst_ref=gains.at[other],
            send_sem=d_s.at[other], recv_sem=d_r.at[other],
            device_id={"dp": other}, device_id_type=MESH,
        )

    for i in range(1, dps):
        other = (dp + i) % dps
        gain_in(other).wait_recv()
        pl.when(is_first)(gain_in(other).wait_send)
    pl.when(sec > 0)(gain_in(dp).wait_recv)
    total = gains[0]
    for at in range(1, dps):
        total = total + gains[at]
    gain_out[...] = total


def hand_on(grads, gains, table, grads_out, gains_out, table_out):
    grads_out[...] = grads[...]
    gains_out[...] = gains[...]
    table_out[...] = table[...]


def per_device(
    stream, cotangent, token_ids, buckets, bias_table, gain, w_query, w_key, w_value, w_out
):
    sections = lax.axis_size("section")
    n = lax.axis_size("mp")
    dps = lax.axis_size("dp")
    micro, seq, width = stream.shape
    heads = bias_table.shape[1]
    inner = w_query.shape[2]
    head_dim = inner // heads
    groups = heads * head_dim // 128
    per = 128 // head_dim
    vmem = pl.BlockSpec(memory_space=pltpu.VMEM)
    hbm = pl.BlockSpec(memory_space=pl.ANY)
    dma = pltpu.SemaphoreType.DMA
    grads, gains, table_grad = pl.pallas_call(
        functools.partial(relay_kernel, sections, n, dps, head_dim),
        out_shape=(
            jax.ShapeDtypeStruct((1, micro, seq, width), bf16),
            jax.ShapeDtypeStruct((1, width), f32),
            jax.ShapeDtypeStruct(bias_table.shape[::-1], f32),
        ),
        in_specs=[vmem, vmem, vmem, vmem, pl.BlockSpec(memory_space=pltpu.SMEM), vmem]
        + [hbm] * 4,
        out_specs=(vmem, vmem, vmem),
        scratch_shapes=[
            pltpu.VMEM(w_query.shape[1:], bf16),
            pltpu.VMEM(w_key.shape[1:], bf16),
            pltpu.VMEM(w_value.shape[1:], bf16),
            pltpu.VMEM(w_out.shape[1:], bf16),
            pltpu.VMEM(w_query.shape[:0:-1], bf16),
            pltpu.VMEM(w_key.shape[:0:-1], bf16),
            pltpu.VMEM(w_value.shape[:0:-1], bf16),
            pltpu.VMEM(w_out.shape[:0:-1], bf16),
            pltpu.VMEM((heads, seq, seq), f32),
            pltpu.VMEM((micro, n, seq, width), bf16),
            pltpu.VMEM((micro, n, seq, inner), bf16),
            pltpu.VMEM((micro, n, seq, inner), bf16),
            pltpu.VMEM((2, micro, n, seq, width), bf16),
            pltpu.VMEM((2, micro, n, 8, seq), f32),
            pltpu.VMEM((micro, seq, width), bf16),
            pltpu.VMEM((micro, n, seq, inner), bf16),
            pltpu.VMEM((micro, n, seq, width), bf16),
            pltpu.VMEM((micro, 8, seq), f32),
            pltpu.VMEM((micro, seq, width), bf16),
            pltpu.VMEM((micro, seq, width), bf16),
            pltpu.VMEM((micro, seq, width), bf16),
            pltpu.VMEM((1, width), f32),
            pltpu.VMEM((1, width), f32),
            pltpu.VMEM((1, width), f32),
            pltpu.VMEM((micro, seq, 3 * inner), f32),
            pltpu.VMEM((micro, seq, 3 * inner), bf16),
            pltpu.VMEM((micro, groups, per * seq, seq), f32),
            pltpu.VMEM((micro, seq, 128), f32),
            pltpu.VMEM((seq, width), f32),
            pltpu.VMEM((seq, inner), f32),
            pltpu.VMEM((seq, 3 * inner), bf16),
            pltpu.VMEM((seq, 128), f32),
            pltpu.VMEM((heads, 8, 2 * seq), f32),
            pltpu.VMEM((sections * dps, max(heads, 8), 2 * seq), f32),
            pltpu.VMEM((dps, 1, width), f32),
            pltpu.VMEM((micro, seq, inner), bf16),
            pltpu.VMEM((micro, seq, width), bf16),
            dma((4,)),
            dma((micro,)),
        ]
        + [dma((micro, n, CHUNKS))] * 8
        + [dma((2, micro, n, CHUNKS)), dma((micro, n)), dma((2, micro, n))]
        + [dma((micro,))] * 4
        + [dma((1,))] * 2
        + [dma((dps,))]
        + [dma((sections * dps,))] * 2
        + [dma((dps,))] * 2
        + [dma((micro, CHUNKS))] * 4
        + [pltpu.SemaphoreType.REGULAR((micro,))],
        compiler_params=pltpu.CompilerParams(
            collective_id=0, has_side_effects=True, vmem_limit_bytes=60 * 1024 * 1024
        ),
    )(
        stream, cotangent, token_ids, buckets, bias_table.T, gain, w_query, w_key, w_value, w_out,
    )
    grads, gains, table_grad = pl.pallas_call(
        hand_on,
        out_shape=(
            jax.ShapeDtypeStruct(grads.shape, bf16),
            jax.ShapeDtypeStruct(gains.shape, f32),
            jax.ShapeDtypeStruct(table_grad.shape, f32),
        ),
        in_specs=[vmem] * 3,
        out_specs=(vmem,) * 3,
    )(grads, gains, table_grad)
    return grads, gains, table_grad.T


def solution(mesh):
    in_specs = (
        P("dp", None, "mp"),
        P("dp", None, "mp"),
        P("dp", None),
        P(),
        P(None, "mp"),
        P("section", None),
        P("section", None, "mp"),
        P("section", None, "mp"),
        P("section", None, "mp"),
        P("section", None, "mp"),
    )
    out_specs = (P("section", "dp", None, "mp"), P("section", "mp"), P(None, "mp"))
    return jax.shard_map(
        per_device, mesh=mesh, in_specs=in_specs, out_specs=out_specs, check_vma=False
    )
```
